128 devices in a mesh: gx: 4 (over x), gy: 4 (over z), gz: 8 (over y, core).
Axes of the slice: x: 4, y: 4, z: 4, core: 2. Of those that a mesh axis runs over, the one named last changes fastest.
Arguments:
- a_blocks: float32 [6656, 7, 128, 128], P(('gx', 'gy', 'gz')), as said below
- block_cols: int32 [6656, 7], P(('gx', 'gy', 'gz')), may hold values from 0 to 363, as said below
- agg_ids: int32 [6656], P(('gx', 'gy', 'gz')), may hold values from 0 to 51, as said below
- agg_counts: int32 [128], P(('gx', 'gy', 'gz')), may hold values from 1 to 52, as said below
- p0_blocks: float32 [6656, 6, 128], P(('gx', 'gy', 'gz')), may hold values from -6 to 6
- start_vec: float32 [6656, 128], P(('gx', 'gy', 'gz'))
Outputs:
- p_blocks: float32 [6656, 7, 6, 128], P(('gx', 'gy', 'gz'))
- p_cols: int32 [6656, 7], P(('gx', 'gy', 'gz'))
- power_vec: float32 [6656, 128], P(('gx', 'gy', 'gz'))
The draws below stay inside these ranges and needn't reach their ends.
Inputs may be any that keep to these rules, and one draw needn't show every extreme that they name: `block_cols`: entry 0 of each block row names the row itself; every neighbour that an entry names exists. `agg_ids`: below the count of the row's own subdomain. `agg_counts`: some subdomain has 52 aggregates. `a_blocks`: block 0 of each block row has a positive diagonal.
All inputs are finite; a program needn't handle non-finite values.
Results may differ from the reference program's by a relative error of at most 0.0003.
Values sent between devices are 32-bit elements; how exact they have to be, the bound alone decides.
A program may use at most 128 MiB of HBM per device.

```python
import jax
import jax.numpy as jnp
from jax import lax

B = 128
NS = 6
K = 7
BR = 52
ITERS = 8
BLOCKS = 6656
N_GX = 4
N_GY = 4
N_GZ = 8


def counts_helper(key):
    device_count = N_GX * N_GY * N_GZ
    per_device = jax.random.randint(jax.random.fold_in(key, 11), (device_count,), 1, BR + 1)
    chosen = jax.random.randint(jax.random.fold_in(key, 12), (), 0, device_count)
    return jnp.where(jnp.arange(device_count) == chosen, BR, per_device).astype(jnp.int32)


def draw_agg_counts(key, part):
    return counts_helper(key)


def draw_agg_ids(key, part):
    counted = jnp.repeat(counts_helper(key), BR)
    return jax.random.randint(jax.random.fold_in(key, 13), (BLOCKS,), 0, counted).astype(jnp.int32)


def draw_block_cols(key, part):
    blocks_all = jnp.arange(BLOCKS)
    device_index = blocks_all // BR
    own_row = blocks_all % BR
    coord_x = device_index // (N_GY * N_GZ)
    coord_y = device_index // N_GZ % N_GY
    coord_z = device_index % N_GZ
    exists = jnp.stack([coord_x > 0, coord_x < N_GX - 1, coord_y > 0, coord_y < N_GY - 1, coord_z > 0, coord_z < N_GZ - 1], axis=1)
    chosen = jax.random.randint(jax.random.fold_in(key, 21), (BLOCKS, 6), 0, 2)
    remote_row = jax.random.randint(jax.random.fold_in(key, 22), (BLOCKS, 6), 0, BR)
    local_row = jax.random.randint(jax.random.fold_in(key, 23), (BLOCKS, 6), 0, BR)
    direction = jnp.arange(6)[None, :]
    use_remote = (chosen == 1) & exists
    picked = jnp.where(use_remote, BR + direction * BR + remote_row, local_row)
    return jnp.concatenate([own_row[:, None], picked], axis=1).astype(jnp.int32)


def draw_a_blocks(key, part):
    device_index = (jnp.arange(BLOCKS) // BR).astype(jnp.float32)
    device_count = N_GX * N_GY * N_GZ
    strength = 0.3 + 1.2 * device_index / max(device_count - 1, 1)
    noise = jax.random.normal(jax.random.fold_in(key, 31), (BLOCKS, K, B, B), jnp.float32)
    diagonal = jax.random.uniform(jax.random.fold_in(key, 32), (BLOCKS, B), jnp.float32, 1.0, 2.0)
    identity = jnp.eye(B, dtype=jnp.float32)
    inner = noise[:, 0] * (0.4 / B ** 0.5) * (1.0 - identity) + identity * diagonal[:, :, None]
    outer = noise[:, 1:] * (strength[:, None, None, None] / (6.0 * B) ** 0.5)
    return jnp.concatenate([inner[:, None], outer], axis=1)


def draw_start_vec(key, part):
    device_index = (jnp.arange(BLOCKS) // BR).astype(jnp.float32)
    device_count = N_GX * N_GY * N_GZ
    ramp = device_index / max(device_count - 1, 1)
    values = jax.random.normal(jax.random.fold_in(key, 41), (BLOCKS, B), jnp.float32)
    return values * (1.0 + 2.0 * ramp)[:, None]


def block_levels(own_key, shape, shards, smallest, top_value):
    loudness, own = 1.0, jax.random.fold_in(own_key, 6)
    for dim, blocks in shards:
        heights = jnp.exp(jax.random.uniform(jax.random.fold_in(own, dim), (blocks,), jnp.float32, smallest / len(shards), top_value / len(shards)))
        loudness = loudness * jnp.repeat(heights, shape[dim] // blocks).reshape([-1 if axis == dim else 1 for axis in range(len(shape))])
    return loudness


def gaussian(rng, shape, deviation, bound, split=(), kind=jnp.bfloat16):
    values = jax.random.normal(rng, shape, jnp.float32) * deviation
    if len(split) > 0:
        values = block_levels(rng, shape, split, -0.22, 0.18) * values
    return jnp.clip(values, min=-bound, max=bound).astype(kind)


def setup_inputs(seed: int = 0) -> dict:
    keys = jax.random.split(jax.random.key(seed), 7)
    a_blocks = draw_a_blocks(jax.random.fold_in(keys[6], 71), 0)
    block_cols = draw_block_cols(jax.random.fold_in(keys[6], 71), 0)
    agg_ids = draw_agg_ids(jax.random.fold_in(keys[6], 71), 0)
    agg_counts = draw_agg_counts(jax.random.fold_in(keys[6], 71), 0)
    p0_blocks = gaussian(keys[4], (BLOCKS, NS, B), 1.0, 6.0, ((0, 128),), jnp.float32)
    start_vec = draw_start_vec(jax.random.fold_in(keys[6], 71), 0)
    return {"a_blocks": a_blocks, "block_cols": block_cols, "agg_ids": agg_ids, "agg_counts": agg_counts, "p0_blocks": p0_blocks, "start_vec": start_vec}


precise_mode = lax.Precision.HIGHEST

def global_rows(block_cols):
    device_count = N_GX * N_GY * N_GZ
    shaped = block_cols.reshape(device_count, BR, K)
    device_index = jnp.arange(device_count, dtype=jnp.int32)[:, None, None]
    strides = jnp.array([-N_GY * N_GZ, N_GY * N_GZ, -N_GZ, N_GZ, -1, 1], dtype=jnp.int32)
    beyond = shaped - BR
    direction = jnp.clip(beyond // BR, 0, 5)
    neighbour_row = beyond % BR
    remote = (device_index + strides[direction]) * BR + neighbour_row
    own_rows = device_index * BR + shaped
    return jnp.where(shaped < BR, own_rows, remote).reshape(device_count * BR, K).astype(jnp.int32)

def reference(a_blocks, block_cols, agg_ids, agg_counts, p0_blocks, start_vec):
    target = global_rows(block_cols)
    diag_values = jnp.diagonal(a_blocks[:, 0], axis1=1, axis2=2)

    def operate(vector):
        picked = vector[target]
        mixed = jnp.einsum('bkij,bkj->bi', a_blocks, picked, precision=precise_mode)
        return mixed / diag_values
    previous = start_vec
    current = start_vec
    for turn_index in range(ITERS):
        previous = current
        current = operate(current)
    last_norm = jnp.sqrt(jnp.sum(current * current))
    spectral = last_norm / jnp.sqrt(jnp.sum(previous * previous))
    power_vec = current * (jnp.sqrt(jnp.float32(BLOCKS * B)) / last_norm)
    damping = 4.0 / (3.0 * spectral)
    picked_p0 = p0_blocks[target]
    product = jnp.einsum('bksj,bkij->bksi', picked_p0, a_blocks, precision=precise_mode)
    smoothed = -(damping / diag_values)[:, None, None, :] * product
    p_blocks = smoothed.at[:, 0].add(p0_blocks)
    offsets = (jnp.cumsum(agg_counts) - agg_counts).astype(jnp.int32)
    p_cols = NS * (offsets[target // BR] + agg_ids[target])
    return (p_blocks, p_cols.astype(jnp.int32), power_vec)
```

```python
import functools

import jax
import jax.numpy as jnp
from jax import lax
from jax.experimental import pallas as pl
from jax.experimental.pallas import tpu as pltpu
from jax.sharding import PartitionSpec as P

ITERS = 8
BR = 52
K = 7
NS = 6
B = 128
G = 4
GROUPS = BR // G
PROWS = 8
NX, NY, NZ = 4, 4, 8
AXES = ("gx", "gy", "gz")
MESH = pl.DeviceIdType.MESH
F32 = jnp.float32


def kernel(
    cols, ids, counts, a_hbm, p0, start,
    prod_hbm, pcols, zlast, norms,
    a_v, x0, x1, acc0, acc1, pt, prod, invd, sq, offs, cg, r1, r2, r3,
    a_sem, xs_sem, xr_sem, ps_sem, pr_sem, out_sem,
    c1s, c1r, c2s, c2r, c3s, c3r, n1s, n1r, n2s, n2r, n3s, n3r,
):
    ix, iy, iz = (lax.axis_index(name) for name in AXES)
    me = (ix * NY + iy) * NZ + iz

    def a_copy(g):
        rows = pl.ds(g * G, G)
        return pltpu.make_async_copy(a_hbm.at[rows], a_v.at[rows], a_sem.at[g])

    for g in range(GROUPS):
        a_copy(g).start()

    def peer_z(d):
        return {"gz": lax.rem(iz + d, NZ)}

    def peer_y(d):
        return {"gy": lax.rem(iy + d, NY)}

    def peer_x(d):
        return {"gx": lax.rem(ix + d, NX)}

    lines = ((peer_z, NZ), (peer_y, NY), (peer_x, NX))

    barrier = pltpu.get_barrier_semaphore()
    for peer, size in lines:
        for d in range(1, size):
            pl.semaphore_signal(barrier, inc=1, device_id=peer(d), device_id_type=MESH)

    def fill(r, carry):
        x0[r] = start[pl.ds(r, 1), :]
        pt[r, 0:NS, :] = p0[r]
        pt[r, NS:8, :] = jnp.full((8 - NS, B), ids[r].astype(F32), F32)
        return carry

    lax.fori_loop(0, BR, fill, 0)
    cg[me] = jnp.full((1, B), counts[0].astype(F32), F32)

    pl.semaphore_wait(barrier, NX + NY + NZ - 3)

    exists = (ix > 0, ix < NX - 1, iy > 0, iy < NY - 1, iz > 0, iz < NZ - 1)
    nearby = (
        {"gx": ix - 1}, {"gx": ix + 1}, {"gy": iy - 1}, {"gy": iy + 1}, {"gz": iz - 1}, {"gz": iz + 1},
    )

    def halo_send(table, send, recv, lo, n):
        for d in range(6):
            @pl.when(exists[d])
            def _(d=d):
                far = d ^ 1
                pltpu.make_async_remote_copy(
                    src_ref=table.at[pl.ds(lo, n)],
                    dst_ref=table.at[pl.ds((far + 1) * BR + lo, n)],
                    send_sem=send.at[d],
                    recv_sem=recv.at[far],
                    device_id=nearby[d],
                    device_id_type=MESH,
                ).start()

    def halo_wait(table, send, recv):
        for d in range(6):
            @pl.when(exists[d])
            def _(d=d):
                copy = pltpu.make_async_remote_copy(
                    src_ref=table.at[pl.ds(0, BR)],
                    dst_ref=table.at[pl.ds((d + 1) * BR, BR)],
                    send_sem=send.at[d],
                    recv_sem=recv.at[d],
                    device_id=nearby[d],
                    device_id_type=MESH,
                )
                copy.wait_recv()
                copy.wait_send()

    def line_copies(ref, peer, size, send, recv):
        return [
            pltpu.make_async_remote_copy(
                src_ref=ref, dst_ref=ref, send_sem=send.at[d - 1], recv_sem=recv.at[d - 1],
                device_id=peer(d), device_id_type=MESH,
            )
            for d in range(1, size)
        ]

    def go(copies):
        for copy in copies:
            copy.start()

    def done(copies):
        for copy in copies:
            copy.wait()

    halo_send(x0, xs_sem.at[0], xr_sem.at[0], 0, BR)
    cg1 = line_copies(cg.at[pl.ds(me, 1)], peer_z, NZ, c1s, c1r)
    cg2 = line_copies(cg.at[pl.ds((ix * NY + iy) * NZ, NZ)], peer_y, NY, c2s, c2r)
    cg3 = line_copies(cg.at[pl.ds(ix * NY * NZ, NY * NZ)], peer_x, NX, c3s, c3r)
    go(cg1)
    halo_send(pt, ps_sem, pr_sem, 0, BR)

    sub = lax.broadcasted_iota(jnp.int32, (B, B), 0)
    lane = lax.broadcasted_iota(jnp.int32, (B, B), 1)

    def multiply(cur, g, acc, first):
        if first:
            a_copy(g).wait()
        for j in range(G):
            b = g * G + j
            total = None
            for k in range(K):
                block = a_v[b, k]
                if first and k == 0:
                    diag = jnp.sum(jnp.where(sub == lane, block, 0.0), axis=0, keepdims=True)
                    invd[b] = 1.0 / diag
                term = block * cur[cols[b, k]]
                total = term if total is None else total + term
            acc[j] = total

    def finish(nxt, g, acc, squares):
        for j in range(G):
            b = g * G + j
            y = jnp.sum(acc[j].T, axis=0, keepdims=True) * invd[b]
            nxt[b] = y
            squares = squares + y * y
        return squares

    def iterate(par, first, last):
        cur, nxt = (x0, x1) if par == 0 else (x1, x0)
        halo_wait(cur, xs_sem.at[par], xr_sem.at[par])
        multiply(cur, 0, acc0, first)

        def pair(i, squares):
            multiply(cur, 2 * i + 1, acc1, first)
            squares = finish(nxt, 2 * i, acc0, squares)
            multiply(cur, 2 * i + 2, acc0, first)
            return finish(nxt, 2 * i + 1, acc1, squares)

        send = functools.partial(halo_send, nxt, xs_sem.at[1 - par], xr_sem.at[1 - par])
        squares = jnp.zeros((1, B), F32)
        half = GROUPS // 4
        squares = lax.fori_loop(0, half, pair, squares)
        if not last:
            send(0, 2 * half * G)
        squares = lax.fori_loop(half, 2 * half, pair, squares)
        if not last:
            send(2 * half * G, 2 * half * G)
        squares = finish(nxt, GROUPS - 1, acc0, squares)
        if not last:
            send(4 * half * G, BR - 4 * half * G)
        return squares

    nt = (((1,), (1,)), ((), ()))

    def p_row(b):
        scale = -invd[b]
        for k in range(K):
            p = pt[cols[b, k]]
            p_hi = p.astype(jnp.bfloat16)
            p_lo = (p - p_hi.astype(F32)).astype(jnp.bfloat16)
            lhs = jnp.concatenate([p_hi, p_lo], axis=0)
            a = a_v[b, k]
            a_hi = a.astype(jnp.bfloat16)
            a_lo = (a - a_hi.astype(F32)).astype(jnp.bfloat16)
            by_hi = lax.dot_general(lhs, a_hi, nt, preferred_element_type=F32)
            by_lo = lax.dot_general(lhs, a_lo, nt, preferred_element_type=F32)
            value = by_hi[0:8] + ((by_hi[8:16] + by_lo[0:8]) + by_lo[8:16])
            prod[b, k] = (value * scale)[0:NS]

    def p_rows(turn):
        first_row = jnp.minimum(PROWS * turn, BR - PROWS)

        def one(r, carry):
            p_row(first_row + r)
            return carry

        lax.fori_loop(0, PROWS, one, 0)

    iterate(0, True, False)
    done(cg1)
    go(cg2)
    halo_wait(pt, ps_sem, pr_sem)

    def two(i, carry):
        p_rows(2 * i)
        iterate(1, False, False)
        p_rows(2 * i + 1)
        sq[...] = iterate(0, False, False)

        @pl.when(i == 0)
        def _():
            done(cg2)
            go(cg3)

        return carry

    lax.fori_loop(0, (ITERS - 2) // 2, two, 0)
    done(cg3)
    p_rows(ITERS - 2)
    out = pltpu.make_async_copy(prod, prod_hbm, out_sem)
    out.start()
    squares = iterate(1, False, True)

    row = lax.broadcasted_iota(jnp.int32, (8, B), 0)
    r1[iz] = jnp.where(row == 0, sq[...], squares)
    red1 = line_copies(r1.at[iz], peer_z, NZ, n1s, n1r)
    go(red1)

    strides = (0, -NY * NZ, NY * NZ, -NZ, NZ, -1, 1)
    table = cg[:, 0, :]
    device = lax.broadcasted_iota(jnp.int32, (NX * NY * NZ, B), 0)
    for f in range(7):
        below = jnp.where(device < me + strides[f], table, 0.0)
        offs[f] = jnp.sum(below, axis=0, keepdims=True)

    def col_row(b):
        spot = lax.broadcasted_iota(jnp.int32, (1, B), 1)
        total = jnp.zeros((1, B), F32)
        for k in range(K):
            c = cols[b, k]
            face = lax.shift_right_logical(c * 1261, 16)
            value = pt[c, NS:NS + 1, :] + offs[face]
            total = jnp.where(spot == k, value, total)
        pcols[b] = (6.0 * total).astype(jnp.int32)

    def col_rows(r, carry):
        for j in range(2):
            col_row(2 * r + j)
        return carry

    lax.fori_loop(0, BR // 2, col_rows, 0)

    def copy_out(r, carry):
        zlast[r] = x0[r]
        return carry

    lax.fori_loop(0, BR, copy_out, 0)

    done(red1)
    r2[iy] = jnp.sum(r1[...], axis=0)
    red2 = line_copies(r2.at[iy], peer_y, NY, n2s, n2r)
    go(red2)
    done(red2)
    r3[ix] = jnp.sum(r2[...], axis=0)
    red3 = line_copies(r3.at[ix], peer_x, NX, n3s, n3r)
    go(red3)
    done(red3)
    total = jnp.sum(r3[...], axis=0)
    norms[...] = jnp.broadcast_to(jnp.sum(total, axis=1, keepdims=True), (8, B))
    out.wait()


def local(a_blocks, block_cols, agg_ids, agg_counts, p0_blocks, start_vec):
    vmem = pl.BlockSpec(memory_space=pltpu.VMEM)
    smem = pl.BlockSpec(memory_space=pltpu.SMEM)
    hbm = pl.BlockSpec(memory_space=pltpu.HBM)
    dma = pltpu.SemaphoreType.DMA
    prod, pcols, zlast, norms = pl.pallas_call(
        kernel,
        out_shape=(
            jax.ShapeDtypeStruct((BR, K, NS, B), F32),
            jax.ShapeDtypeStruct((BR, 1, B), jnp.int32),
            jax.ShapeDtypeStruct((BR, 1, B), F32),
            jax.ShapeDtypeStruct((8, B), F32),
        ),
        in_specs=[smem, smem, smem, hbm, vmem, vmem],
        out_specs=(hbm, vmem, vmem, vmem),
        scratch_shapes=[
            pltpu.VMEM((BR, K, B, B), F32),
            pltpu.VMEM((7 * BR, 1, B), F32),
            pltpu.VMEM((7 * BR, 1, B), F32),
            pltpu.VMEM((G, B, B), F32),
            pltpu.VMEM((G, B, B), F32),
            pltpu.VMEM((7 * BR, 8, B), F32),
            pltpu.VMEM((BR, K, NS, B), F32),
            pltpu.VMEM((BR, 1, B), F32),
            pltpu.VMEM((1, B), F32),
            pltpu.VMEM((7, 1, B), F32),
            pltpu.VMEM((NX * NY * NZ, 1, B), F32),
            pltpu.VMEM((NZ, 8, B), F32),
            pltpu.VMEM((NY, 8, B), F32),
            pltpu.VMEM((NX, 8, B), F32),
            dma((GROUPS,)),
            dma((2, 6)),
            dma((2, 6)),
            dma((6,)),
            dma((6,)),
            dma(()),
            dma((NZ - 1,)), dma((NZ - 1,)),
            dma((NY - 1,)), dma((NY - 1,)),
            dma((NX - 1,)), dma((NX - 1,)),
            dma((NZ - 1,)), dma((NZ - 1,)),
            dma((NY - 1,)), dma((NY - 1,)),
            dma((NX - 1,)), dma((NX - 1,)),
        ],
        compiler_params=pltpu.CompilerParams(
            collective_id=0, has_side_effects=True, vmem_limit_bytes=56 * 1024 * 1024
        ),
        name="prolongator",
    )(block_cols, agg_ids, agg_counts, a_blocks, p0_blocks, start_vec)
    last_norm = jnp.sqrt(norms[1, 0])
    spectral = last_norm / jnp.sqrt(norms[0, 0])
    entries = NX * NY * NZ * BR * B
    power_vec = zlast.reshape(BR, B) * (jnp.sqrt(F32(entries)) / last_norm)
    damping = 4.0 / (3.0 * spectral)
    own = jnp.pad(p0_blocks[:, None], ((0, 0), (0, K - 1), (0, 0), (0, 0)))
    p_blocks = damping * prod + own
    p_cols = pcols.reshape(BR, B)[:, :K]
    return p_blocks, p_cols, power_vec


def solution(mesh):
    placed = (
        P(AXES, None, None, None),
        P(AXES, None),
        P(AXES),
        P(AXES),
        P(AXES, None, None),
        P(AXES, None),
    )
    return jax.shard_map(
        local,
        mesh=mesh,
        in_specs=placed,
        out_specs=(P(AXES, None, None, None), P(AXES, None), P(AXES, None)),
        check_vma=False,
    )
```

```python
import functools

import jax
import jax.numpy as jnp
from jax import lax
from jax.experimental import pallas as pl
from jax.experimental.pallas import tpu as pltpu
from jax.sharding import PartitionSpec as P

ITERS = 8
BR = 52
K = 7
NS = 6
B = 128
G = 8
HALF = 4
FULL = BR // G
PROWS = 7
NX, NY, NZ = 4, 4, 8
AXES = ("gx", "gy", "gz")
MESH = pl.DeviceIdType.MESH
F32 = jnp.float32


def kernel(
    cols_hbm, ids_hbm, counts, a_hbm, p0_hbm, start_hbm,
    prod_out, pcols_out, z_out, norms_out,
    cols, ids, p0, start, a_v, x0, x1, acc, pt, prod, invd, own, sq, offs, cg, r1, r2, r3,
    coltab, pcols, zlast, norms,
    in_sem, a_sem, xs_sem, xr_sem, ps_sem, pr_sem, out_sem,
    c1s, c1r, c2s, c2r, c3s, c3r, n1s, n1r, n2s, n2r, n3s, n3r,
):
    ix, iy, iz = (lax.axis_index(name) for name in AXES)
    me = (ix * NY + iy) * NZ + iz

    small = [
        pltpu.make_async_copy(far, near, in_sem.at[i])
        for i, (far, near) in enumerate(
            ((start_hbm, start), (ids_hbm, ids), (p0_hbm, p0), (cols_hbm, cols))
        )
    ]
    for copy in small:
        copy.start()

    def a_copy(g):
        rows = pl.ds(g * HALF, HALF)
        return pltpu.make_async_copy(a_hbm.at[rows], a_v.at[rows], a_sem.at[g])

    for g in range(BR // HALF):
        a_copy(g).start()

    def peer_z(d):
        return {"gz": lax.rem(iz + d, NZ)}

    def peer_y(d):
        return {"gy": lax.rem(iy + d, NY)}

    def peer_x(d):
        return {"gx": lax.rem(ix + d, NX)}

    lines = ((peer_z, NZ), (peer_y, NY), (peer_x, NX))

    barrier = pltpu.get_barrier_semaphore()
    for peer, size in lines:
        for d in range(1, size):
            pl.semaphore_signal(barrier, inc=1, device_id=peer(d), device_id_type=MESH)

    small[0].wait()
    for r in range(BR):
        x0[r] = start[r:r + 1, :]
    cg[me] = jnp.full((1, B), counts[0].astype(F32), F32)

    pl.semaphore_wait(barrier, NX + NY + NZ - 3)

    exists = (ix > 0, ix < NX - 1, iy > 0, iy < NY - 1, iz > 0, iz < NZ - 1)
    nearby = (
        {"gx": ix - 1}, {"gx": ix + 1}, {"gy": iy - 1}, {"gy": iy + 1}, {"gz": iz - 1}, {"gz": iz + 1},
    )

    def halo_send(table, send, recv, lo, n):
        for d in range(6):
            @pl.when(exists[d])
            def _(d=d):
                far = d ^ 1
                pltpu.make_async_remote_copy(
                    src_ref=table.at[pl.ds(lo, n)],
                    dst_ref=table.at[pl.ds((far + 1) * BR + lo, n)],
                    send_sem=send.at[d],
                    recv_sem=recv.at[far],
                    device_id=nearby[d],
                    device_id_type=MESH,
                ).start()

    def halo_wait(table, send, recv):
        for d in range(6):
            @pl.when(exists[d])
            def _(d=d):
                copy = pltpu.make_async_remote_copy(
                    src_ref=table.at[pl.ds(0, BR)],
                    dst_ref=table.at[pl.ds((d + 1) * BR, BR)],
                    send_sem=send.at[d],
                    recv_sem=recv.at[d],
                    device_id=nearby[d],
                    device_id_type=MESH,
                )
                copy.wait_recv()
                copy.wait_send()

    def line_copies(ref, peer, size, send, recv):
        return [
            pltpu.make_async_remote_copy(
                src_ref=ref, dst_ref=ref, send_sem=send.at[d - 1], recv_sem=recv.at[d - 1],
                device_id=peer(d), device_id_type=MESH,
            )
            for d in range(1, size)
        ]

    def go(copies):
        for copy in copies:
            copy.start()

    def done(copies):
        for copy in copies:
            copy.wait()

    halo_send(x0, xs_sem.at[0], xr_sem.at[0], 0, BR)
    cg1 = line_copies(cg.at[pl.ds(me, 1)], peer_z, NZ, c1s, c1r)
    cg2 = line_copies(cg.at[pl.ds((ix * NY + iy) * NZ, NZ)], peer_y, NY, c2s, c2r)
    cg3 = line_copies(cg.at[pl.ds(ix * NY * NZ, NY * NZ)], peer_x, NX, c3s, c3r)
    go(cg1)

    small[1].wait()
    small[2].wait()

    def fill(r, carry):
        for s in range(NS):
            pt[r, s:s + 1, :] = p0[s, pl.ds(r, 1), :]
        pt[r, NS:8, :] = jnp.full((8 - NS, B), ids[r].astype(F32), F32)
        return carry

    lax.fori_loop(0, BR, fill, 0)
    halo_send(pt, ps_sem, pr_sem, 0, BR)
    small[3].wait()

    sub = lax.broadcasted_iota(jnp.int32, (B, B), 0)
    lane = lax.broadcasted_iota(jnp.int32, (B, B), 1)

    def lane_sums(block):
        return jnp.sum(block.T, axis=0, keepdims=True)

    def multiply(cur, b, first):
        total = None
        for k in range(0 if first else 1, K):
            block = a_v[b, k]
            if first and k == 0:
                diag = jnp.sum(jnp.where(sub == lane, block, 0.0), axis=0, keepdims=True)
                invd[b] = 1.0 / diag
            term = block * cur[cols[k, b]]
            total = term if total is None else total + term
        return total

    def finish(nxt, b, j, first, squares):
        y = lane_sums(acc[j])
        if not first:
            y = y + own[b]
        y = y * invd[b]
        nxt[b] = y
        return squares + y * y

    def iterate(par, first, last):
        cur, nxt = (x0, x1) if par == 0 else (x1, x0)
        halo_wait(cur, xs_sem.at[par], xr_sem.at[par])
        if first:
            a_copy(0).wait()
            a_copy(1).wait()
        for j in range(G):
            acc[j] = multiply(cur, j, first)

        def stage(g, squares):
            if first:
                a_copy(2 * g).wait()
                a_copy(2 * g + 1).wait()
            for j in range(G):
                squares = finish(nxt, (g - 1) * G + j, j, first, squares)
                acc[j] = multiply(cur, g * G + j, first)
            return squares

        send = functools.partial(halo_send, nxt, xs_sem.at[1 - par], xr_sem.at[1 - par])
        squares = jnp.zeros((1, B), F32)
        squares = lax.fori_loop(1, 4, stage, squares)
        if not last:
            send(0, 3 * G)
        squares = lax.fori_loop(4, FULL, stage, squares)
        if first:
            a_copy(2 * FULL).wait()
        for j in range(G):
            squares = finish(nxt, (FULL - 1) * G + j, j, first, squares)
            if j < BR - FULL * G:
                acc[j] = multiply(cur, FULL * G + j, first)
        if not last:
            send(3 * G, 3 * G)
        for j in range(BR - FULL * G):
            squares = finish(nxt, FULL * G + j, j, first, squares)
        if not last:
            send(FULL * G, BR - FULL * G)
        return squares

    nt = (((1,), (1,)), ((), ()))

    def halves(value):
        high = value.astype(jnp.bfloat16)
        return high, (value - high.astype(F32)).astype(jnp.bfloat16)

    def p_row(b):
        scale = -invd[b]
        for k in range(K):
            p_hi, p_lo = halves(pt[cols[k, b]])
            p_all = jnp.concatenate([p_hi, p_lo], axis=0)
            a_all = jnp.concatenate(halves(a_v[b, k]), axis=1)
            value = lax.dot_general(
                jnp.concatenate([p_all, p_all], axis=1), a_all, nt, preferred_element_type=F32
            )
            value = (value[0:8] + value[8:16]) * scale
            for s in range(NS):
                prod[k, s, pl.ds(b, 1), :] = value[s:s + 1]

    def between(cur, turn):
        def one(r, carry):
            p_row(turn * PROWS + r)
            lo = jnp.minimum(r * G, BR - G)
            for j in range(G):
                own[lo + j] = lane_sums(a_v[lo + j, 0] * cur[lo + j])
            return carry

        lax.fori_loop(0, PROWS, one, 0)

    iterate(0, True, False)
    done(cg1)
    go(cg2)
    halo_wait(pt, ps_sem, pr_sem)

    def two(i, carry):
        between(x1, 2 * i)
        iterate(1, False, False)
        between(x0, 2 * i + 1)
        sq[...] = iterate(0, False, False)

        @pl.when(i == 0)
        def _():
            done(cg2)
            go(cg3)

        return carry

    lax.fori_loop(0, (ITERS - 2) // 2, two, 0)
    done(cg3)
    between(x1, ITERS - 2)
    squares = iterate(1, False, True)

    row = lax.broadcasted_iota(jnp.int32, (8, B), 0)
    r1[iz] = jnp.where(row == 0, sq[...], squares)
    red1 = line_copies(r1.at[iz], peer_z, NZ, n1s, n1r)
    go(red1)

    for b in range(PROWS * (ITERS - 1), BR):
        p_row(b)
    out = [pltpu.make_async_copy(prod, prod_out, out_sem.at[0])]
    out[0].start()

    done(red1)
    r2[iy] = jnp.sum(r1[...], axis=0)
    red2 = line_copies(r2.at[iy], peer_y, NY, n2s, n2r)
    go(red2)

    strides = (0, -NY * NZ, NY * NZ, -NZ, NZ, -1, 1)
    table = cg[:, 0, :]
    device = lax.broadcasted_iota(jnp.int32, (NX * NY * NZ, B), 0)
    for f in range(7):
        below = jnp.where(device < me + strides[f], table, 0.0)
        offs[f] = jnp.sum(below, axis=0, keepdims=True)

    def col_rows(r, carry):
        spot = lax.broadcasted_iota(jnp.int32, (1, B), 1)
        for j in range(4):
            b = 4 * r + j
            total = jnp.zeros((1, B), F32)
            for k in range(K):
                c = cols[k, b]
                face = lax.shift_right_logical(c * 1261, 16)
                value = pt[c, NS:NS + 1, :] + offs[face]
                total = jnp.where(spot == k, value, total)
            coltab[pl.ds(b, 1), :] = 6.0 * total
            zlast[pl.ds(b, 1), :] = x0[b]
        return carry

    lax.fori_loop(0, BR // 4, col_rows, 0)
    pcols[...] = coltab[...].T[0:K, 0:BR].astype(jnp.int32)
    out.append(pltpu.make_async_copy(pcols, pcols_out, out_sem.at[1]))
    out.append(pltpu.make_async_copy(zlast, z_out, out_sem.at[2]))
    out[1].start()
    out[2].start()

    done(red2)
    r3[ix] = jnp.sum(r2[...], axis=0)
    red3 = line_copies(r3.at[ix], peer_x, NX, n3s, n3r)
    go(red3)
    done(red3)
    total = jnp.sum(r3[...], axis=0)
    norms[...] = jnp.broadcast_to(jnp.sum(total, axis=1, keepdims=True), (8, B))
    out.append(pltpu.make_async_copy(norms, norms_out, out_sem.at[3]))
    out[3].start()
    for copy in out:
        copy.wait()


def scaled(prod, pcols, z, norms, p0, p_blocks, p_cols, power_vec):
    last_norm = jnp.sqrt(norms[1:2, :])
    spectral = last_norm / jnp.sqrt(norms[0:1, :])
    entries = NX * NY * NZ * BR * B
    power_vec[...] = z[...] * (jnp.sqrt(F32(entries)) / last_norm)
    damping = 4.0 / (3.0 * spectral)
    for k in range(K):
        for s in range(NS):
            value = damping * prod[k, s]
            p_blocks[k, s] = value + p0[s] if k == 0 else value
    p_cols[...] = pcols[...]


def local(a_blocks, block_cols, agg_ids, agg_counts, p0_blocks, start_vec):
    vmem = pl.BlockSpec(memory_space=pltpu.VMEM)
    hbm = pl.BlockSpec(memory_space=pltpu.HBM)
    anywhere = pl.BlockSpec(memory_space=pl.ANY)
    dma = pltpu.SemaphoreType.DMA
    p0_turned = jnp.transpose(p0_blocks, (1, 0, 2))
    shapes = (
        jax.ShapeDtypeStruct((K, NS, BR, B), F32),
        jax.ShapeDtypeStruct((K, BR), jnp.int32),
        jax.ShapeDtypeStruct((BR, B), F32),
    )
    prod, pcols, zlast, norms = pl.pallas_call(
        kernel,
        out_shape=(*shapes, jax.ShapeDtypeStruct((8, B), F32)),
        in_specs=[hbm, hbm, pl.BlockSpec(memory_space=pltpu.SMEM), hbm, hbm, hbm],
        out_specs=(anywhere,) * 4,
        scratch_shapes=[
            pltpu.SMEM((K, BR), jnp.int32),
            pltpu.SMEM((BR,), jnp.int32),
            pltpu.VMEM((NS, BR, B), F32),
            pltpu.VMEM((BR, B), F32),
            pltpu.VMEM((BR, K, B, B), F32),
            pltpu.VMEM((7 * BR, 1, B), F32),
            pltpu.VMEM((7 * BR, 1, B), F32),
            pltpu.VMEM((G, B, B), F32),
            pltpu.VMEM((7 * BR, 8, B), F32),
            pltpu.VMEM((K, NS, BR, B), F32),
            pltpu.VMEM((BR, 1, B), F32),
            pltpu.VMEM((BR, 1, B), F32),
            pltpu.VMEM((1, B), F32),
            pltpu.VMEM((7, 1, B), F32),
            pltpu.VMEM((NX * NY * NZ, 1, B), F32),
            pltpu.VMEM((NZ, 8, B), F32),
            pltpu.VMEM((NY, 8, B), F32),
            pltpu.VMEM((NX, 8, B), F32),
            pltpu.VMEM((B, B), F32),
            pltpu.VMEM((K, BR), jnp.int32),
            pltpu.VMEM((BR, B), F32),
            pltpu.VMEM((8, B), F32),
            dma((4,)),
            dma((BR // HALF,)),
            dma((2, 6)),
            dma((2, 6)),
            dma((6,)),
            dma((6,)),
            dma((4,)),
            dma((NZ - 1,)), dma((NZ - 1,)),
            dma((NY - 1,)), dma((NY - 1,)),
            dma((NX - 1,)), dma((NX - 1,)),
            dma((NZ - 1,)), dma((NZ - 1,)),
            dma((NY - 1,)), dma((NY - 1,)),
            dma((NX - 1,)), dma((NX - 1,)),
        ],
        compiler_params=pltpu.CompilerParams(
            collective_id=0, has_side_effects=True, vmem_limit_bytes=67_043_328
        ),
        name="prolongator",
    )(block_cols.T, agg_ids, agg_counts, a_blocks, p0_turned, start_vec)
    p_blocks, p_cols, power_vec = pl.pallas_call(
        scaled,
        out_shape=shapes,
        in_specs=[vmem] * 5,
        out_specs=(vmem,) * 3,
        name="scaled",
    )(prod, pcols, zlast, norms, p0_turned)
    return jnp.transpose(p_blocks, (2, 0, 1, 3)), p_cols.T, power_vec


def solution(mesh):
    placed = (
        P(AXES, None, None, None),
        P(AXES, None),
        P(AXES),
        P(AXES),
        P(AXES, None, None),
        P(AXES, None),
    )
    return jax.shard_map(
        local,
        mesh=mesh,
        in_specs=placed,
        out_specs=(P(AXES, None, None, None), P(AXES, None), P(AXES, None)),
        check_vma=False,
    )
```

```python
import functools

import jax
import jax.numpy as jnp
from jax import lax
from jax.experimental import pallas as pl
from jax.experimental.pallas import tpu as pltpu
from jax.sharding import PartitionSpec as P

ITERS = 8
BR = 52
K = 7
NS = 6
B = 128
G = 8
HALF = 4
FULL = BR // G
PROWS = 7
NX, NY, NZ = 4, 4, 8
AXES = ("gx", "gy", "gz")
MESH = pl.DeviceIdType.MESH
F32 = jnp.float32


def kernel(
    cols_hbm, ids_hbm, counts, a_hbm, p0_hbm, start_hbm,
    prod_out, pcols_out, z_out, norms_out,
    cols, ids, p0, start, a_v, x0, x1, acc, pt, prod, invd, own, sq, offs, cg, r1, r2,
    coltab, pcols, zlast, norms,
    in_sem, a_sem, xs_sem, xr_sem, ps_sem, pr_sem, out_sem,
    c1s, c1r, c2s, c2r, n1s, n1r, n2s, n2r,
):
    ix, iy, iz = (lax.axis_index(name) for name in AXES)
    me = (ix * NY + iy) * NZ + iz

    small = [
        pltpu.make_async_copy(far, near, in_sem.at[i])
        for i, (far, near) in enumerate(
            ((start_hbm, start), (ids_hbm, ids), (p0_hbm, p0), (cols_hbm, cols))
        )
    ]
    for copy in small:
        copy.start()
    early = 3

    def a_copy(g):
        rows = pl.ds(g * HALF, HALF)
        return pltpu.make_async_copy(a_hbm.at[rows], a_v.at[rows], a_sem.at[g])


    for g in range(early):
        a_copy(g).start()

    def peer_z(d):
        return {"gz": lax.rem(iz + d, NZ)}

    def peer_xy(d):
        return {"gx": lax.rem(ix + d // NY, NX), "gy": lax.rem(iy + d, NY)}

    lines = ((peer_z, NZ), (peer_xy, NX * NY))

    barrier = pltpu.get_barrier_semaphore()
    for peer, size in lines:
        for d in range(1, size):
            pl.semaphore_signal(barrier, inc=1, device_id=peer(d), device_id_type=MESH)

    for copy in small:
        copy.wait()
    for g in range(early, BR // HALF):
        a_copy(g).start()
    for r in range(BR):
        x0[r] = start[r:r + 1, :]
    cg[me] = jnp.full((1, B), counts[0].astype(F32), F32)

    pl.semaphore_wait(barrier, NX * NY + NZ - 2)

    exists = (ix > 0, ix < NX - 1, iy > 0, iy < NY - 1, iz > 0, iz < NZ - 1)
    nearby = (
        {"gx": ix - 1}, {"gx": ix + 1}, {"gy": iy - 1}, {"gy": iy + 1}, {"gz": iz - 1}, {"gz": iz + 1},
    )

    def halo_send(table, send, recv, lo, n):
        for d in range(6):
            @pl.when(exists[d])
            def _(d=d):
                far = d ^ 1
                pltpu.make_async_remote_copy(
                    src_ref=table.at[pl.ds(lo, n)],
                    dst_ref=table.at[pl.ds((far + 1) * BR + lo, n)],
                    send_sem=send.at[d],
                    recv_sem=recv.at[far],
                    device_id=nearby[d],
                    device_id_type=MESH,
                ).start()

    def halo_wait(table, send, recv):
        for d in range(6):
            @pl.when(exists[d])
            def _(d=d):
                copy = pltpu.make_async_remote_copy(
                    src_ref=table.at[pl.ds(0, BR)],
                    dst_ref=table.at[pl.ds((d + 1) * BR, BR)],
                    send_sem=send.at[d],
                    recv_sem=recv.at[d],
                    device_id=nearby[d],
                    device_id_type=MESH,
                )
                copy.wait_recv()
                copy.wait_send()

    def line_copies(ref, peer, size, send, recv):
        return [
            pltpu.make_async_remote_copy(
                src_ref=ref, dst_ref=ref, send_sem=send.at[d - 1], recv_sem=recv.at[d - 1],
                device_id=peer(d), device_id_type=MESH,
            )
            for d in range(1, size)
        ]

    def go(copies):
        for copy in copies:
            copy.start()

    def done(copies):
        for copy in copies:
            copy.wait()

    halo_send(x0, xs_sem.at[0], xr_sem.at[0], 0, BR)
    cg1 = line_copies(cg.at[pl.ds(me, 1)], peer_z, NZ, c1s, c1r)
    cg2 = line_copies(cg.at[pl.ds((ix * NY + iy) * NZ, NZ)], peer_xy, NX * NY, c2s, c2r)
    go(cg1)


    def fill(r, carry):
        for s in range(NS):
            pt[r, s:s + 1, :] = p0[s, pl.ds(r, 1), :]
        pt[r, NS:8, :] = jnp.full((8 - NS, B), ids[r].astype(F32), F32)
        return carry

    lax.fori_loop(0, BR, fill, 0)
    halo_send(pt, ps_sem, pr_sem, 0, BR)

    sub = lax.broadcasted_iota(jnp.int32, (B, B), 0)
    lane = lax.broadcasted_iota(jnp.int32, (B, B), 1)

    def lane_sums(block):
        return jnp.sum(block.T, axis=0, keepdims=True)

    def multiply(cur, b, first):
        total = None
        for k in range(0 if first else 1, K):
            block = a_v[b, k]
            if first and k == 0:
                diag = jnp.sum(jnp.where(sub == lane, block, 0.0), axis=0, keepdims=True)
                invd[b] = 1.0 / diag
            term = block * cur[cols[k, b]]
            total = term if total is None else total + term
        return total

    def finish(nxt, b, j, first, squares):
        y = lane_sums(acc[j])
        if not first:
            y = y + own[b]
        y = y * invd[b]
        nxt[b] = y
        return squares + y * y

    def iterate(par, first, last):
        cur, nxt = (x0, x1) if par == 0 else (x1, x0)
        halo_wait(cur, xs_sem.at[par], xr_sem.at[par])
        if first:
            a_copy(0).wait()
            a_copy(1).wait()
        for j in range(G):
            acc[j] = multiply(cur, j, first)

        def stage(g, squares):
            if first:
                a_copy(2 * g).wait()
                a_copy(2 * g + 1).wait()
            for j in range(G):
                squares = finish(nxt, (g - 1) * G + j, j, first, squares)
                acc[j] = multiply(cur, g * G + j, first)
            return squares

        send = functools.partial(halo_send, nxt, xs_sem.at[1 - par], xr_sem.at[1 - par])
        squares = jnp.zeros((1, B), F32)
        squares = lax.fori_loop(1, 4, stage, squares)
        if not last:
            send(0, 3 * G)
        squares = lax.fori_loop(4, FULL, stage, squares)
        if first:
            a_copy(2 * FULL).wait()
        for j in range(G):
            squares = finish(nxt, (FULL - 1) * G + j, j, first, squares)
            if j < BR - FULL * G:
                acc[j] = multiply(cur, FULL * G + j, first)
        if not last:
            send(3 * G, 3 * G)
        for j in range(BR - FULL * G):
            squares = finish(nxt, FULL * G + j, j, first, squares)
        if not last:
            send(FULL * G, BR - FULL * G)
        return squares

    nt = (((1,), (1,)), ((), ()))

    def halves(value):
        high = value.astype(jnp.bfloat16)
        return high, (value - high.astype(F32)).astype(jnp.bfloat16)

    def p_row(b):
        scale = -invd[b]
        for k in range(K):
            p_hi, p_lo = halves(pt[cols[k, b]])
            p_all = jnp.concatenate([p_hi, p_lo], axis=0)
            a_all = jnp.concatenate(halves(a_v[b, k]), axis=1)
            value = lax.dot_general(
                jnp.concatenate([p_all, p_all], axis=1), a_all, nt, preferred_element_type=F32
            )
            value = (value[0:8] + value[8:16]) * scale
            for s in range(NS):
                prod[k, s, pl.ds(b, 1), :] = value[s:s + 1]

    def between(cur, turn):
        def one(r, carry):
            p_row(turn * PROWS + r)
            lo = jnp.minimum(r * G, BR - G)
            for j in range(G):
                own[lo + j] = lane_sums(a_v[lo + j, 0] * cur[lo + j])
            return carry

        lax.fori_loop(0, PROWS, one, 0)

    iterate(0, True, False)
    done(cg1)
    go(cg2)
    halo_wait(pt, ps_sem, pr_sem)

    def two(i, carry):
        between(x1, 2 * i)
        iterate(1, False, False)
        between(x0, 2 * i + 1)
        sq[...] = iterate(0, False, False)

        return carry

    lax.fori_loop(0, (ITERS - 2) // 2, two, 0)
    done(cg2)
    between(x1, ITERS - 2)
    squares = iterate(1, False, True)

    row = lax.broadcasted_iota(jnp.int32, (8, B), 0)
    r1[iz] = jnp.where(row == 0, sq[...], squares)
    red1 = line_copies(r1.at[iz], peer_z, NZ, n1s, n1r)
    go(red1)

    for b in range(PROWS * (ITERS - 1), BR):
        p_row(b)
    out = [pltpu.make_async_copy(prod, prod_out, out_sem.at[0])]
    out[0].start()

    done(red1)
    r2[ix * NY + iy] = jnp.sum(r1[...], axis=0)
    red2 = line_copies(r2.at[ix * NY + iy], peer_xy, NX * NY, n2s, n2r)
    go(red2)

    strides = (0, -NY * NZ, NY * NZ, -NZ, NZ, -1, 1)
    table = cg[:, 0, :]
    device = lax.broadcasted_iota(jnp.int32, (NX * NY * NZ, B), 0)
    for f in range(7):
        below = jnp.where(device < me + strides[f], table, 0.0)
        offs[f] = jnp.sum(below, axis=0, keepdims=True)

    def col_rows(r, carry):
        spot = lax.broadcasted_iota(jnp.int32, (1, B), 1)
        for j in range(4):
            b = 4 * r + j
            total = jnp.zeros((1, B), F32)
            for k in range(K):
                c = cols[k, b]
                face = lax.shift_right_logical(c * 1261, 16)
                value = pt[c, NS:NS + 1, :] + offs[face]
                total = jnp.where(spot == k, value, total)
            coltab[pl.ds(b, 1), :] = 6.0 * total
            zlast[pl.ds(b, 1), :] = x0[b]
        return carry

    lax.fori_loop(0, BR // 4, col_rows, 0)
    pcols[...] = coltab[...].T[0:K, 0:BR].astype(jnp.int32)
    out.append(pltpu.make_async_copy(pcols, pcols_out, out_sem.at[1]))
    out.append(pltpu.make_async_copy(zlast, z_out, out_sem.at[2]))
    out[1].start()
    out[2].start()

    done(red2)
    total = jnp.sum(r2[...], axis=0)
    norms[...] = jnp.broadcast_to(jnp.sum(total, axis=1, keepdims=True), (8, B))
    out.append(pltpu.make_async_copy(norms, norms_out, out_sem.at[3]))
    out[3].start()
    for copy in out:
        copy.wait()


def scaled(prod, pcols, z, norms, p0, p_blocks, p_cols, power_vec):
    last_norm = jnp.sqrt(norms[1:2, :])
    spectral = last_norm / jnp.sqrt(norms[0:1, :])
    entries = NX * NY * NZ * BR * B
    power_vec[...] = z[...] * (jnp.sqrt(F32(entries)) / last_norm)
    damping = 4.0 / (3.0 * spectral)
    for k in range(K):
        for s in range(NS):
            value = damping * prod[k, s]
            p_blocks[k, s] = value + p0[s] if k == 0 else value
    p_cols[...] = pcols[...]


def local(a_blocks, block_cols, agg_ids, agg_counts, p0_blocks, start_vec):
    vmem = pl.BlockSpec(memory_space=pltpu.VMEM)
    hbm = pl.BlockSpec(memory_space=pltpu.HBM)
    anywhere = pl.BlockSpec(memory_space=pl.ANY)
    dma = pltpu.SemaphoreType.DMA
    p0_turned = jnp.transpose(p0_blocks, (1, 0, 2))
    shapes = (
        jax.ShapeDtypeStruct((K, NS, BR, B), F32),
        jax.ShapeDtypeStruct((K, BR), jnp.int32),
        jax.ShapeDtypeStruct((BR, B), F32),
    )
    prod, pcols, zlast, norms = pl.pallas_call(
        kernel,
        out_shape=(*shapes, jax.ShapeDtypeStruct((8, B), F32)),
        in_specs=[hbm, hbm, pl.BlockSpec(memory_space=pltpu.SMEM), hbm, hbm, hbm],
        out_specs=(anywhere,) * 4,
        scratch_shapes=[
            pltpu.SMEM((K, BR), jnp.int32),
            pltpu.SMEM((BR,), jnp.int32),
            pltpu.VMEM((NS, BR, B), F32),
            pltpu.VMEM((BR, B), F32),
            pltpu.VMEM((BR, K, B, B), F32),
            pltpu.VMEM((7 * BR, 1, B), F32),
            pltpu.VMEM((7 * BR, 1, B), F32),
            pltpu.VMEM((G, B, B), F32),
            pltpu.VMEM((7 * BR, 8, B), F32),
            pltpu.VMEM((K, NS, BR, B), F32),
            pltpu.VMEM((BR, 1, B), F32),
            pltpu.VMEM((BR, 1, B), F32),
            pltpu.VMEM((1, B), F32),
            pltpu.VMEM((7, 1, B), F32),
            pltpu.VMEM((NX * NY * NZ, 1, B), F32),
            pltpu.VMEM((NZ, 8, B), F32),
            pltpu.VMEM((NX * NY, 8, B), F32),
            pltpu.VMEM((B, B), F32),
            pltpu.VMEM((K, BR), jnp.int32),
            pltpu.VMEM((BR, B), F32),
            pltpu.VMEM((8, B), F32),
            dma((4,)),
            dma((BR // HALF,)),
            dma((2, 6)),
            dma((2, 6)),
            dma((6,)),
            dma((6,)),
            dma((4,)),
            dma((NZ - 1,)), dma((NZ - 1,)),
            dma((NX * NY - 1,)), dma((NX * NY - 1,)),
            dma((NZ - 1,)), dma((NZ - 1,)),
            dma((NX * NY - 1,)), dma((NX * NY - 1,)),
        ],
        compiler_params=pltpu.CompilerParams(
            collective_id=0, has_side_effects=True, vmem_limit_bytes=67_043_328
        ),
        name="prolongator",
    )(block_cols.T, agg_ids, agg_counts, a_blocks, p0_turned, start_vec)
    p_blocks, p_cols, power_vec = pl.pallas_call(
        scaled,
        out_shape=shapes,
        in_specs=[vmem] * 5,
        out_specs=(vmem,) * 3,
        name="scaled",
    )(prod, pcols, zlast, norms, p0_turned)
    return jnp.transpose(p_blocks, (2, 0, 1, 3)), p_cols.T, power_vec


def solution(mesh):
    placed = (
        P(AXES, None, None, None),
        P(AXES, None),
        P(AXES),
        P(AXES),
        P(AXES, None, None),
        P(AXES, None),
    )
    return jax.shard_map(
        local,
        mesh=mesh,
        in_specs=placed,
        out_specs=(P(AXES, None, None, None), P(AXES, None), P(AXES, None)),
        check_vma=False,
    )
```

```python
import functools

import jax
import jax.numpy as jnp
from jax import lax
from jax.experimental import pallas as pl
from jax.experimental.pallas import tpu as pltpu
from jax.sharding import PartitionSpec as P

ITERS = 8
BR = 52
K = 7
NS = 6
B = 128
G = 8
HALF = 4
FULL = BR // G
PROWS = 10
OWN = 6
NX, NY, NZ = 4, 4, 8
AXES = ("gx", "gy", "gz")
MESH = pl.DeviceIdType.MESH
F32 = jnp.float32


def kernel(
    cols_hbm, ids_hbm, counts, a_hbm, p0_hbm, start_hbm,
    prod_out, pcols_out, z_out, norms_out,
    cols, ids, p0, start, a_v, x0, x1, acc, pt, prod, invd, own, sq, offs, cg, r1, r2,
    coltab, pcols, zlast, norms,
    in_sem, a_sem, xs_sem, xr_sem, ps_sem, pr_sem, out_sem,
    c1s, c1r, c2s, c2r, n1s, n1r, n2s, n2r,
):
    ix, iy, iz = (lax.axis_index(name) for name in AXES)
    me = (ix * NY + iy) * NZ + iz

    small = [
        pltpu.make_async_copy(far, near, in_sem.at[i])
        for i, (far, near) in enumerate(
            ((start_hbm, start), (ids_hbm, ids), (p0_hbm, p0), (cols_hbm, cols))
        )
    ]
    for copy in small:
        copy.start()
    early = 3

    def a_copy(g):
        rows = pl.ds(g * HALF, HALF)
        return pltpu.make_async_copy(a_hbm.at[rows], a_v.at[rows], a_sem.at[g])


    for g in range(early):
        a_copy(g).start()

    def peer_z(d):
        return {"gz": lax.rem(iz + d, NZ)}

    def peer_xy(d):
        return {"gx": lax.rem(ix + d // NY, NX), "gy": lax.rem(iy + d, NY)}

    lines = ((peer_z, NZ), (peer_xy, NX * NY))

    barrier = pltpu.get_barrier_semaphore()
    for peer, size in lines:
        for d in range(1, size):
            pl.semaphore_signal(barrier, inc=1, device_id=peer(d), device_id_type=MESH)

    for copy in small:
        copy.wait()
    for g in range(early, BR // HALF):
        a_copy(g).start()
    for r in range(BR):
        x0[r] = start[r:r + 1, :]
    cg[me] = jnp.full((1, B), counts[0].astype(F32), F32)

    pl.semaphore_wait(barrier, NX * NY + NZ - 2)

    exists = (ix > 0, ix < NX - 1, iy > 0, iy < NY - 1, iz > 0, iz < NZ - 1)
    nearby = (
        {"gx": ix - 1}, {"gx": ix + 1}, {"gy": iy - 1}, {"gy": iy + 1}, {"gz": iz - 1}, {"gz": iz + 1},
    )

    def halo_send(table, send, recv, lo, n):
        for d in range(6):
            @pl.when(exists[d])
            def _(d=d):
                far = d ^ 1
                pltpu.make_async_remote_copy(
                    src_ref=table.at[pl.ds(lo, n)],
                    dst_ref=table.at[pl.ds((far + 1) * BR + lo, n)],
                    send_sem=send.at[d],
                    recv_sem=recv.at[far],
                    device_id=nearby[d],
                    device_id_type=MESH,
                ).start()

    def halo_wait(table, send, recv):
        for d in range(6):
            @pl.when(exists[d])
            def _(d=d):
                copy = pltpu.make_async_remote_copy(
                    src_ref=table.at[pl.ds(0, BR)],
                    dst_ref=table.at[pl.ds((d + 1) * BR, BR)],
                    send_sem=send.at[d],
                    recv_sem=recv.at[d],
                    device_id=nearby[d],
                    device_id_type=MESH,
                )
                copy.wait_recv()
                copy.wait_send()

    def line_copies(ref, peer, size, send, recv):
        return [
            pltpu.make_async_remote_copy(
                src_ref=ref, dst_ref=ref, send_sem=send.at[d - 1], recv_sem=recv.at[d - 1],
                device_id=peer(d), device_id_type=MESH,
            )
            for d in range(1, size)
        ]

    def go(copies):
        for copy in copies:
            copy.start()

    def done(copies):
        for copy in copies:
            copy.wait()

    halo_send(x0, xs_sem.at[0], xr_sem.at[0], 0, BR)
    cg1 = line_copies(cg.at[pl.ds(me, 1)], peer_z, NZ, c1s, c1r)
    cg2 = line_copies(cg.at[pl.ds((ix * NY + iy) * NZ, NZ)], peer_xy, NX * NY, c2s, c2r)
    go(cg1)


    def fill(r, carry):
        for j in range(4):
            b = 4 * r + j
            for s in range(NS):
                pt[b, s:s + 1, :] = p0[s, pl.ds(b, 1), :]
            pt[b, NS:8, :] = jnp.full((8 - NS, B), ids[b].astype(F32), F32)
        return carry

    sub = lax.broadcasted_iota(jnp.int32, (B, B), 0)
    lane = lax.broadcasted_iota(jnp.int32, (B, B), 1)

    def lane_sums(block):
        return jnp.sum(block.T, axis=0, keepdims=True)

    def multiply(cur, b, first):
        total = None
        for k in range(0 if first else 1, K):
            block = a_v[b, k]
            if first and k == 0:
                diag = jnp.sum(jnp.where(sub == lane, block, 0.0), axis=0, keepdims=True)
                invd[b] = 1.0 / diag
            term = block * cur[cols[k, b]]
            total = term if total is None else total + term
        return total

    def finish(nxt, b, j, first, squares):
        y = lane_sums(acc[j])
        if not first:
            y = y + own[b]
        y = y * invd[b]
        nxt[b] = y
        return squares + y * y

    def iterate(par, first, last):
        cur, nxt = (x0, x1) if par == 0 else (x1, x0)
        halo_wait(cur, xs_sem.at[par], xr_sem.at[par])
        send = functools.partial(halo_send, nxt, xs_sem.at[1 - par], xr_sem.at[1 - par])
        if not first:
            squares = jnp.zeros((1, B), F32)
            for lo, hi in ((0, 32), (32, BR)):
                for b in range(lo, hi):
                    y = (lane_sums(multiply(cur, b, first)) + own[b]) * invd[b]
                    nxt[b] = y
                    squares = squares + y * y
                if not last:
                    send(lo, hi - lo)
            return squares
        if first:
            a_copy(0).wait()
            a_copy(1).wait()
        for j in range(G):
            acc[j] = multiply(cur, j, first)

        def stage(g, squares):
            if first:
                a_copy(2 * g).wait()
                a_copy(2 * g + 1).wait()
            for j in range(G):
                squares = finish(nxt, (g - 1) * G + j, j, first, squares)
                acc[j] = multiply(cur, g * G + j, first)
            return squares

        squares = jnp.zeros((1, B), F32)
        squares = lax.fori_loop(1, 4, stage, squares)
        if not last:
            send(0, 3 * G)
        squares = lax.fori_loop(4, FULL, stage, squares)
        if first:
            a_copy(2 * FULL).wait()
        for j in range(G):
            squares = finish(nxt, (FULL - 1) * G + j, j, first, squares)
            if j < BR - FULL * G:
                acc[j] = multiply(cur, FULL * G + j, first)
        if not last:
            send(3 * G, 3 * G)
        for j in range(BR - FULL * G):
            squares = finish(nxt, FULL * G + j, j, first, squares)
        if not last:
            send(FULL * G, BR - FULL * G)
        return squares

    nt = (((1,), (1,)), ((), ()))

    def halves(value):
        high = value.astype(jnp.bfloat16)
        return high, (value - high.astype(F32)).astype(jnp.bfloat16)

    def p_row(b):
        scale = -invd[b]
        for k in range(K):
            p_hi, p_lo = halves(pt[cols[k, b]])
            p_all = jnp.concatenate([p_hi, p_lo], axis=0)
            a_all = jnp.concatenate(halves(a_v[b, k]), axis=1)
            value = lax.dot_general(
                jnp.concatenate([p_all, p_all], axis=1), a_all, nt, preferred_element_type=F32
            )
            value = (value[0:8] + value[8:16]) * scale
            for s in range(NS):
                prod[k, s, pl.ds(b, 1), :] = value[s:s + 1]

    def own_rows(cur, lo, n):
        for j in range(n):
            own[lo + j] = lane_sums(a_v[lo + j, 0] * cur[lo + j])

    def own_only(cur):
        def one(r, carry):
            own_rows(cur, r * 13, 13)
            return carry

        lax.fori_loop(0, BR // 13, one, 0)

    def between(cur, turn):
        def one(r, carry):
            p_row(turn * PROWS + r)
            own_rows(cur, jnp.minimum(r * OWN, BR - OWN), OWN)
            return carry

        lax.fori_loop(0, PROWS, one, 0)

    iterate(0, True, False)
    done(cg1)
    go(cg2)

    def two(i, carry):
        @pl.when(i == 0)
        def _():
            lax.fori_loop(0, BR // 4, fill, 0)
            halo_send(pt, ps_sem, pr_sem, 0, BR // 2)
            own_only(x1)

        @pl.when(i > 0)
        def _():
            between(x1, 2 * i - 2)

        iterate(1, False, False)

        @pl.when(i == 0)
        def _():
            halo_send(pt, ps_sem, pr_sem, BR // 2, BR // 2)
            own_only(x0)

        @pl.when(i > 0)
        def _():
            between(x0, 2 * i - 1)

        sq[0] = iterate(0, False, False)

        @pl.when(i == 0)
        def _():
            halo_wait(pt, ps_sem, pr_sem)

        return carry

    lax.fori_loop(0, (ITERS - 2) // 2, two, 0)
    done(cg2)
    between(x1, ITERS - 4)
    sq[1] = iterate(1, False, True)

    both = jnp.sum(sq[...], axis=2, keepdims=True)
    spot = lax.broadcasted_iota(jnp.int32, (1, B), 1)
    r1[iz] = jnp.where(spot < B // 2, both[0], both[1])
    red1 = line_copies(r1.at[iz], peer_z, NZ, n1s, n1r)
    go(red1)

    for b in range(PROWS * (ITERS - 3), BR):
        p_row(b)
    out = [pltpu.make_async_copy(prod, prod_out, out_sem.at[0])]
    out[0].start()

    done(red1)
    r2[ix * NY + iy] = jnp.sum(r1[...], axis=0)
    red2 = line_copies(r2.at[ix * NY + iy], peer_xy, NX * NY, n2s, n2r)
    go(red2)

    strides = (0, -NY * NZ, NY * NZ, -NZ, NZ, -1, 1)
    table = cg[:, 0, :]
    device = lax.broadcasted_iota(jnp.int32, (NX * NY * NZ, B), 0)
    for f in range(7):
        below = jnp.where(device < me + strides[f], table, 0.0)
        offs[f] = jnp.sum(below, axis=0, keepdims=True)

    def col_rows(r, carry):
        for j in range(4):
            b = 4 * r + j
            total = jnp.zeros((1, B), F32)
            for k in range(K):
                c = cols[k, b]
                face = lax.shift_right_logical(c * 1261, 16)
                value = pt[c, NS:NS + 1, :] + offs[face]
                total = jnp.where(spot == k, value, total)
            coltab[pl.ds(b, 1), :] = 6.0 * total
            zlast[pl.ds(b, 1), :] = x0[b]
        return carry

    lax.fori_loop(0, BR // 4, col_rows, 0)
    pcols[...] = coltab[...].T[0:K, 0:BR].astype(jnp.int32)
    out.append(pltpu.make_async_copy(pcols, pcols_out, out_sem.at[1]))
    out.append(pltpu.make_async_copy(zlast, z_out, out_sem.at[2]))
    out[1].start()
    out[2].start()

    done(red2)
    total = jnp.sum(r2[...], axis=0)
    norms[...] = total
    out.append(pltpu.make_async_copy(norms, norms_out, out_sem.at[3]))
    out[3].start()
    for copy in out:
        copy.wait()


def scaled(prod, pcols, z, norms, p0, p_blocks, p_cols, power_vec):
    last_norm = jnp.sqrt(norms[:, B - 1:B])
    spectral = last_norm / jnp.sqrt(norms[:, 0:1])
    entries = NX * NY * NZ * BR * B
    power_vec[...] = z[...] * (jnp.sqrt(F32(entries)) / last_norm)
    damping = 4.0 / (3.0 * spectral)
    for k in range(K):
        for s in range(NS):
            value = damping * prod[k, s]
            p_blocks[k, s] = value + p0[s] if k == 0 else value
    p_cols[...] = pcols[...]


def local(a_blocks, block_cols, agg_ids, agg_counts, p0_blocks, start_vec):
    vmem = pl.BlockSpec(memory_space=pltpu.VMEM)
    hbm = pl.BlockSpec(memory_space=pltpu.HBM)
    anywhere = pl.BlockSpec(memory_space=pl.ANY)
    dma = pltpu.SemaphoreType.DMA
    p0_turned = jnp.transpose(p0_blocks, (1, 0, 2))
    shapes = (
        jax.ShapeDtypeStruct((K, NS, BR, B), F32),
        jax.ShapeDtypeStruct((K, BR), jnp.int32),
        jax.ShapeDtypeStruct((BR, B), F32),
    )
    prod, pcols, zlast, norms = pl.pallas_call(
        kernel,
        out_shape=(*shapes, jax.ShapeDtypeStruct((1, B), F32)),
        in_specs=[hbm, hbm, pl.BlockSpec(memory_space=pltpu.SMEM), hbm, hbm, hbm],
        out_specs=(anywhere,) * 4,
        scratch_shapes=[
            pltpu.SMEM((K, BR), jnp.int32),
            pltpu.SMEM((BR,), jnp.int32),
            pltpu.VMEM((NS, BR, B), F32),
            pltpu.VMEM((BR, B), F32),
            pltpu.VMEM((BR, K, B, B), F32),
            pltpu.VMEM((7 * BR, 1, B), F32),
            pltpu.VMEM((7 * BR, 1, B), F32),
            pltpu.VMEM((G, B, B), F32),
            pltpu.VMEM((7 * BR, 8, B), F32),
            pltpu.VMEM((K, NS, BR, B), F32),
            pltpu.VMEM((BR, 1, B), F32),
            pltpu.VMEM((BR, 1, B), F32),
            pltpu.VMEM((2, 1, B), F32),
            pltpu.VMEM((7, 1, B), F32),
            pltpu.VMEM((NX * NY * NZ, 1, B), F32),
            pltpu.VMEM((NZ, 1, B), F32),
            pltpu.VMEM((NX * NY, 1, B), F32),
            pltpu.VMEM((B, B), F32),
            pltpu.VMEM((K, BR), jnp.int32),
            pltpu.VMEM((BR, B), F32),
            pltpu.VMEM((1, B), F32),
            dma((4,)),
            dma((BR // HALF,)),
            dma((2, 6)),
            dma((2, 6)),
            dma((6,)),
            dma((6,)),
            dma((4,)),
            dma((NZ - 1,)), dma((NZ - 1,)),
            dma((NX * NY - 1,)), dma((NX * NY - 1,)),
            dma((NZ - 1,)), dma((NZ - 1,)),
            dma((NX * NY - 1,)), dma((NX * NY - 1,)),
        ],
        compiler_params=pltpu.CompilerParams(
            collective_id=0, has_side_effects=True, vmem_limit_bytes=67_043_328
        ),
        name="prolongator",
    )(block_cols.T, agg_ids, agg_counts, a_blocks, p0_turned, start_vec)
    p_blocks, p_cols, power_vec = pl.pallas_call(
        scaled,
        out_shape=shapes,
        in_specs=[vmem] * 5,
        out_specs=(vmem,) * 3,
        name="scaled",
    )(prod, pcols, zlast, norms, p0_turned)
    return jnp.transpose(p_blocks, (2, 0, 1, 3)), p_cols.T, power_vec


def solution(mesh):
    placed = (
        P(AXES, None, None, None),
        P(AXES, None),
        P(AXES),
        P(AXES),
        P(AXES, None, None),
        P(AXES, None),
    )
    return jax.shard_map(
        local,
        mesh=mesh,
        in_specs=placed,
        out_specs=(P(AXES, None, None, None), P(AXES, None), P(AXES, None)),
        check_vma=False,
    )
```

```python
import functools

import jax
import jax.numpy as jnp
from jax import lax
from jax.experimental import pallas as pl
from jax.experimental.pallas import tpu as pltpu
from jax.sharding import PartitionSpec as P

ITERS = 8
BR = 52
K = 7
NS = 6
B = 128
G = 8
HALF = 4
FULL = BR // G
PROWS = 10
OWN = 6
NX, NY, NZ = 4, 4, 8
AXES = ("gx", "gy", "gz")
MESH = pl.DeviceIdType.MESH
F32 = jnp.float32


def kernel(
    cols_hbm, ids_hbm, counts, a_hbm, p0_hbm, start_hbm,
    prod_out, pcols_out, z_out, norms_out,
    cols, ids, p0, start, a_v, x0, x1, acc, pt, prod, invd, own, sq, offs, cg, r1, r2,
    coltab, pcols, zlast, norms,
    in_sem, a_sem, xs_sem, xr_sem, ps_sem, pr_sem, out_sem,
    c1s, c1r, c2s, c2r, n1s, n1r, n2s, n2r,
):
    ix, iy, iz = (lax.axis_index(name) for name in AXES)
    me = (ix * NY + iy) * NZ + iz

    small = [
        pltpu.make_async_copy(far, near, in_sem.at[i])
        for i, (far, near) in enumerate(
            ((start_hbm, start), (ids_hbm, ids), (p0_hbm, p0), (cols_hbm, cols))
        )
    ]
    for copy in small:
        copy.start()
    early = 3

    def a_copy(g):
        rows = pl.ds(g * HALF, HALF)
        return pltpu.make_async_copy(a_hbm.at[rows], a_v.at[rows], a_sem.at[g])


    for g in range(early):
        a_copy(g).start()

    def peer_z(d):
        return {"gz": lax.rem(iz + d, NZ)}

    def peer_xy(d):
        return {"gx": lax.rem(ix + d // NY, NX), "gy": lax.rem(iy + d, NY)}

    lines = ((peer_z, NZ), (peer_xy, NX * NY))

    barrier = pltpu.get_barrier_semaphore()
    for peer, size in lines:
        for d in range(1, size):
            pl.semaphore_signal(barrier, inc=1, device_id=peer(d), device_id_type=MESH)

    for copy in small:
        copy.wait()
    for g in range(early, BR // HALF):
        a_copy(g).start()
    for r in range(BR):
        x0[r] = start[r:r + 1, :]
    cg[me] = jnp.full((1, B), counts[0].astype(F32), F32)

    pl.semaphore_wait(barrier, NX * NY + NZ - 2)

    exists = (ix > 0, ix < NX - 1, iy > 0, iy < NY - 1, iz > 0, iz < NZ - 1)
    nearby = (
        {"gx": ix - 1}, {"gx": ix + 1}, {"gy": iy - 1}, {"gy": iy + 1}, {"gz": iz - 1}, {"gz": iz + 1},
    )

    def halo_send(table, send, recv, lo, n):
        for d in range(6):
            @pl.when(exists[d])
            def _(d=d):
                far = d ^ 1
                pltpu.make_async_remote_copy(
                    src_ref=table.at[pl.ds(lo, n)],
                    dst_ref=table.at[pl.ds((far + 1) * BR + lo, n)],
                    send_sem=send.at[d],
                    recv_sem=recv.at[far],
                    device_id=nearby[d],
                    device_id_type=MESH,
                ).start()

    def halo_wait(table, send, recv):
        for d in range(6):
            @pl.when(exists[d])
            def _(d=d):
                copy = pltpu.make_async_remote_copy(
                    src_ref=table.at[pl.ds(0, BR)],
                    dst_ref=table.at[pl.ds((d + 1) * BR, BR)],
                    send_sem=send.at[d],
                    recv_sem=recv.at[d],
                    device_id=nearby[d],
                    device_id_type=MESH,
                )
                copy.wait_recv()
                copy.wait_send()

    def line_copies(ref, peer, size, send, recv):
        return [
            pltpu.make_async_remote_copy(
                src_ref=ref, dst_ref=ref, send_sem=send.at[d - 1], recv_sem=recv.at[d - 1],
                device_id=peer(d), device_id_type=MESH,
            )
            for d in range(1, size)
        ]

    def go(copies):
        for copy in copies:
            copy.start()

    def done(copies):
        for copy in copies:
            copy.wait()

    halo_send(x0, xs_sem.at[0], xr_sem.at[0], 0, BR)
    cg1 = line_copies(cg.at[pl.ds(me, 1)], peer_z, NZ, c1s, c1r)
    cg2 = line_copies(cg.at[pl.ds((ix * NY + iy) * NZ, NZ)], peer_xy, NX * NY, c2s, c2r)
    go(cg1)


    def fill(r, carry):
        for j in range(4):
            b = 4 * r + j
            for s in range(NS):
                pt[b, s:s + 1, :] = p0[s, pl.ds(b, 1), :]
            pt[b, NS:8, :] = jnp.full((8 - NS, B), ids[b].astype(F32), F32)
        return carry

    sub = lax.broadcasted_iota(jnp.int32, (B, B), 0)
    lane = lax.broadcasted_iota(jnp.int32, (B, B), 1)

    def lane_sums(block):
        return jnp.sum(block.T, axis=0, keepdims=True)

    def multiply(cur, b, first):
        total = None
        for k in range(0 if first else 1, K):
            block = a_v[b, k]
            if first and k == 0:
                diag = jnp.sum(jnp.where(sub == lane, block, 0.0), axis=0, keepdims=True)
                invd[b] = 1.0 / diag
            term = block * cur[cols[k, b]]
            total = term if total is None else total + term
        return total

    def finish(nxt, b, j, first, squares):
        y = lane_sums(acc[j])
        if not first:
            y = y + own[b]
        y = y * invd[b]
        nxt[b] = y
        return squares + y * y

    def iterate(par, first, last):
        cur, nxt = (x0, x1) if par == 0 else (x1, x0)
        halo_wait(cur, xs_sem.at[par], xr_sem.at[par])
        send = functools.partial(halo_send, nxt, xs_sem.at[1 - par], xr_sem.at[1 - par])
        if not first:
            squares = jnp.zeros((1, B), F32)
            for lo, hi in ((0, 40), (40, BR)):
                for b in range(lo, hi):
                    y = (lane_sums(multiply(cur, b, first)) + own[b]) * invd[b]
                    nxt[b] = y
                    squares = squares + y * y
                if not last:
                    send(lo, hi - lo)
            return squares
        if first:
            a_copy(0).wait()
            a_copy(1).wait()
        for j in range(G):
            acc[j] = multiply(cur, j, first)

        def stage(g, squares):
            if first:
                a_copy(2 * g).wait()
                a_copy(2 * g + 1).wait()
            for j in range(G):
                squares = finish(nxt, (g - 1) * G + j, j, first, squares)
                acc[j] = multiply(cur, g * G + j, first)
            return squares

        squares = jnp.zeros((1, B), F32)
        squares = lax.fori_loop(1, 4, stage, squares)
        if not last:
            send(0, 3 * G)
        squares = lax.fori_loop(4, FULL, stage, squares)
        if first:
            a_copy(2 * FULL).wait()
        for j in range(G):
            squares = finish(nxt, (FULL - 1) * G + j, j, first, squares)
            if j < BR - FULL * G:
                acc[j] = multiply(cur, FULL * G + j, first)
        if not last:
            send(3 * G, 3 * G)
        for j in range(BR - FULL * G):
            squares = finish(nxt, FULL * G + j, j, first, squares)
        if not last:
            send(FULL * G, BR - FULL * G)
        return squares

    nt = (((1,), (1,)), ((), ()))

    def halves(value):
        high = value.astype(jnp.bfloat16)
        return high, (value - high.astype(F32)).astype(jnp.bfloat16)

    def p_row(b):
        scale = -invd[b]
        for k in range(K):
            p_hi, p_lo = halves(pt[cols[k, b]])
            p_all = jnp.concatenate([p_hi, p_lo], axis=0)
            a_all = jnp.concatenate(halves(a_v[b, k]), axis=1)
            value = lax.dot_general(
                jnp.concatenate([p_all, p_all], axis=1), a_all, nt, preferred_element_type=F32
            )
            value = (value[0:8] + value[8:16]) * scale
            for s in range(NS):
                prod[k, s, pl.ds(b, 1), :] = value[s:s + 1]

    def own_rows(cur, lo, n):
        for j in range(n):
            own[lo + j] = lane_sums(a_v[lo + j, 0] * cur[lo + j])

    def own_only(cur):
        def one(r, carry):
            own_rows(cur, r * 13, 13)
            return carry

        lax.fori_loop(0, BR // 13, one, 0)

    def between(cur, turn):
        def one(r, carry):
            p_row(turn * PROWS + r)
            own_rows(cur, jnp.minimum(r * OWN, BR - OWN), OWN)
            return carry

        lax.fori_loop(0, PROWS, one, 0)

    iterate(0, True, False)
    done(cg1)
    go(cg2)

    def two(i, carry):
        @pl.when(i == 0)
        def _():
            lax.fori_loop(0, BR // 4, fill, 0)
            halo_send(pt, ps_sem, pr_sem, 0, BR // 2)
            own_only(x1)

        @pl.when(i > 0)
        def _():
            between(x1, 2 * i - 2)

        iterate(1, False, False)

        @pl.when(i == 0)
        def _():
            halo_send(pt, ps_sem, pr_sem, BR // 2, BR // 2)
            own_only(x0)

        @pl.when(i > 0)
        def _():
            between(x0, 2 * i - 1)

        sq[0] = iterate(0, False, False)

        @pl.when(i == 0)
        def _():
            halo_wait(pt, ps_sem, pr_sem)

        return carry

    lax.fori_loop(0, (ITERS - 2) // 2, two, 0)
    done(cg2)
    between(x1, ITERS - 4)
    sq[1] = iterate(1, False, True)

    both = jnp.sum(sq[...], axis=2, keepdims=True)
    spot = lax.broadcasted_iota(jnp.int32, (1, B), 1)
    r1[iz] = jnp.where(spot < B // 2, both[0], both[1])
    red1 = line_copies(r1.at[iz], peer_z, NZ, n1s, n1r)
    go(red1)

    for b in range(PROWS * (ITERS - 3), BR):
        p_row(b)
    out = [pltpu.make_async_copy(prod, prod_out, out_sem.at[0])]
    out[0].start()

    done(red1)
    r2[ix * NY + iy] = jnp.sum(r1[...], axis=0)
    red2 = line_copies(r2.at[ix * NY + iy], peer_xy, NX * NY, n2s, n2r)
    go(red2)

    strides = (0, -NY * NZ, NY * NZ, -NZ, NZ, -1, 1)
    table = cg[:, 0, :]
    device = lax.broadcasted_iota(jnp.int32, (NX * NY * NZ, B), 0)
    for f in range(7):
        below = jnp.where(device < me + strides[f], table, 0.0)
        offs[f] = jnp.sum(below, axis=0, keepdims=True)

    def col_rows(r, carry):
        for j in range(4):
            b = 4 * r + j
            total = jnp.zeros((1, B), F32)
            for k in range(K):
                c = cols[k, b]
                face = lax.shift_right_logical(c * 1261, 16)
                value = pt[c, NS:NS + 1, :] + offs[face]
                total = jnp.where(spot == k, value, total)
            coltab[pl.ds(b, 1), :] = 6.0 * total
            zlast[pl.ds(b, 1), :] = x0[b]
        return carry

    lax.fori_loop(0, BR // 4, col_rows, 0)
    pcols[...] = coltab[...].T[0:K, 0:BR].astype(jnp.int32)
    out.append(pltpu.make_async_copy(pcols, pcols_out, out_sem.at[1]))
    out.append(pltpu.make_async_copy(zlast, z_out, out_sem.at[2]))
    out[1].start()
    out[2].start()

    done(red2)
    total = jnp.sum(r2[...], axis=0)
    norms[...] = total
    out.append(pltpu.make_async_copy(norms, norms_out, out_sem.at[3]))
    out[3].start()
    for copy in out:
        copy.wait()


def scaled(
    prod, pcols, z, norms, p0, p_blocks, p_cols, power_vec,
    prod_v, pcols_v, z_v, norms_v, p0_v, in_sem, out_sem,
):
    def taken(i, far, near):
        return pltpu.make_async_copy(far, near, in_sem.at[i])

    def given(i, near, far):
        return pltpu.make_async_copy(near, far, out_sem.at[i])

    whole = [
        taken(K + i, far, near)
        for i, (far, near) in enumerate(((norms, norms_v), (p0, p0_v), (z, z_v), (pcols, pcols_v)))
    ]
    parts = [taken(k, prod.at[k], prod_v.at[k]) for k in range(K)]
    for copy in whole[:2] + parts + whole[2:]:
        copy.start()
    whole[0].wait()
    last_norm = jnp.sqrt(norms_v[:, B - 1:B])
    spectral = last_norm / jnp.sqrt(norms_v[:, 0:1])
    entries = NX * NY * NZ * BR * B
    rescale = jnp.sqrt(F32(entries)) / last_norm
    damping = 4.0 / (3.0 * spectral)
    whole[1].wait()
    results = []
    for k in range(K):
        parts[k].wait()
        for s in range(NS):
            value = damping * prod_v[k, s]
            prod_v[k, s] = value + p0_v[s] if k == 0 else value
        results.append(given(k, prod_v.at[k], p_blocks.at[k]))
        results[k].start()
    whole[2].wait()
    z_v[...] = z_v[...] * rescale
    results.append(given(K, z_v, power_vec))
    results[K].start()
    whole[3].wait()
    results.append(given(K + 1, pcols_v, p_cols))
    results[K + 1].start()
    for copy in results:
        copy.wait()


def local(a_blocks, block_cols, agg_ids, agg_counts, p0_blocks, start_vec):
    hbm = pl.BlockSpec(memory_space=pltpu.HBM)
    anywhere = pl.BlockSpec(memory_space=pl.ANY)
    dma = pltpu.SemaphoreType.DMA
    p0_turned = jnp.transpose(p0_blocks, (1, 0, 2))
    shapes = (
        jax.ShapeDtypeStruct((K, NS, BR, B), F32),
        jax.ShapeDtypeStruct((K, BR), jnp.int32),
        jax.ShapeDtypeStruct((BR, B), F32),
    )
    prod, pcols, zlast, norms = pl.pallas_call(
        kernel,
        out_shape=(*shapes, jax.ShapeDtypeStruct((1, B), F32)),
        in_specs=[hbm, hbm, pl.BlockSpec(memory_space=pltpu.SMEM), hbm, hbm, hbm],
        out_specs=(anywhere,) * 4,
        scratch_shapes=[
            pltpu.SMEM((K, BR), jnp.int32),
            pltpu.SMEM((BR,), jnp.int32),
            pltpu.VMEM((NS, BR, B), F32),
            pltpu.VMEM((BR, B), F32),
            pltpu.VMEM((BR, K, B, B), F32),
            pltpu.VMEM((7 * BR, 1, B), F32),
            pltpu.VMEM((7 * BR, 1, B), F32),
            pltpu.VMEM((G, B, B), F32),
            pltpu.VMEM((7 * BR, 8, B), F32),
            pltpu.VMEM((K, NS, BR, B), F32),
            pltpu.VMEM((BR, 1, B), F32),
            pltpu.VMEM((BR, 1, B), F32),
            pltpu.VMEM((2, 1, B), F32),
            pltpu.VMEM((7, 1, B), F32),
            pltpu.VMEM((NX * NY * NZ, 1, B), F32),
            pltpu.VMEM((NZ, 1, B), F32),
            pltpu.VMEM((NX * NY, 1, B), F32),
            pltpu.VMEM((B, B), F32),
            pltpu.VMEM((K, BR), jnp.int32),
            pltpu.VMEM((BR, B), F32),
            pltpu.VMEM((1, B), F32),
            dma((4,)),
            dma((BR // HALF,)),
            dma((2, 6)),
            dma((2, 6)),
            dma((6,)),
            dma((6,)),
            dma((4,)),
            dma((NZ - 1,)), dma((NZ - 1,)),
            dma((NX * NY - 1,)), dma((NX * NY - 1,)),
            dma((NZ - 1,)), dma((NZ - 1,)),
            dma((NX * NY - 1,)), dma((NX * NY - 1,)),
        ],
        compiler_params=pltpu.CompilerParams(
            collective_id=0, has_side_effects=True, vmem_limit_bytes=67_043_328
        ),
        name="prolongator",
    )(block_cols.T, agg_ids, agg_counts, a_blocks, p0_turned, start_vec)
    p_blocks, p_cols, power_vec = pl.pallas_call(
        scaled,
        out_shape=shapes,
        in_specs=[hbm] * 5,
        out_specs=(hbm,) * 3,
        scratch_shapes=[
            pltpu.VMEM((K, NS, BR, B), F32),
            pltpu.VMEM((K, BR), jnp.int32),
            pltpu.VMEM((BR, B), F32),
            pltpu.VMEM((1, B), F32),
            pltpu.VMEM((NS, BR, B), F32),
            dma((K + 4,)),
            dma((K + 2,)),
        ],
        compiler_params=pltpu.CompilerParams(vmem_limit_bytes=67_043_328),
        name="scaled",
    )(prod, pcols, zlast, norms, p0_turned)
    return jnp.transpose(p_blocks, (2, 0, 1, 3)), p_cols.T, power_vec


def solution(mesh):
    placed = (
        P(AXES, None, None, None),
        P(AXES, None),
        P(AXES),
        P(AXES),
        P(AXES, None, None),
        P(AXES, None),
    )
    return jax.shard_map(
        local,
        mesh=mesh,
        in_specs=placed,
        out_specs=(P(AXES, None, None, None), P(AXES, None), P(AXES, None)),
        check_vma=False,
    )
```

```python
import functools

import jax
import jax.numpy as jnp
from jax import lax
from jax.experimental import pallas as pl
from jax.experimental.pallas import tpu as pltpu
from jax.sharding import PartitionSpec as P

ITERS = 8
BR = 52
K = 7
NS = 6
B = 128
G = 8
HALF = 4
FULL = BR // G
PROWS = 10
OWN = 6
NX, NY, NZ = 4, 4, 8
AXES = ("gx", "gy", "gz")
MESH = pl.DeviceIdType.MESH
F32 = jnp.float32


def kernel(
    cols_hbm, ids_hbm, counts, a_hbm, p0_hbm, start_hbm,
    prod_out, pcols_out, z_out, norms_out,
    cols, ids, p0, start, a_v, x0, x1, acc, pt, prod, invd, own, sq, offs, cg, r1, r2,
    coltab, pcols, zlast, norms,
    in_sem, a_sem, xs_sem, xr_sem, ps_sem, pr_sem, out_sem,
    c1s, c1r, c2s, c2r, n1s, n1r, n2s, n2r,
):
    ix, iy, iz = (lax.axis_index(name) for name in AXES)
    me = (ix * NY + iy) * NZ + iz

    small = [
        pltpu.make_async_copy(far, near, in_sem.at[i])
        for i, (far, near) in enumerate(
            ((start_hbm, start), (ids_hbm, ids), (p0_hbm, p0), (cols_hbm, cols))
        )
    ]
    for copy in small:
        copy.start()
    early = 3

    def a_copy(g):
        rows = pl.ds(g * HALF, HALF)
        return pltpu.make_async_copy(a_hbm.at[rows], a_v.at[rows], a_sem.at[g])


    for g in range(early):
        a_copy(g).start()

    def peer_z(d):
        return {"gz": lax.rem(iz + d, NZ)}

    def peer_xy(d):
        return {"gx": lax.rem(ix + d // NY, NX), "gy": lax.rem(iy + d, NY)}

    lines = ((peer_z, NZ), (peer_xy, NX * NY))

    barrier = pltpu.get_barrier_semaphore()
    for peer, size in lines:
        for d in range(1, size):
            pl.semaphore_signal(barrier, inc=1, device_id=peer(d), device_id_type=MESH)

    for copy in small:
        copy.wait()
    for g in range(early, BR // HALF):
        a_copy(g).start()
    for r in range(BR):
        x0[r] = start[r:r + 1, :]
    cg[me] = jnp.full((1, B), counts[0].astype(F32), F32)

    pl.semaphore_wait(barrier, NX * NY + NZ - 2)

    exists = (ix > 0, ix < NX - 1, iy > 0, iy < NY - 1, iz > 0, iz < NZ - 1)
    nearby = (
        {"gx": ix - 1}, {"gx": ix + 1}, {"gy": iy - 1}, {"gy": iy + 1}, {"gz": iz - 1}, {"gz": iz + 1},
    )

    def halo_send(table, send, recv, lo, n):
        for d in range(6):
            @pl.when(exists[d])
            def _(d=d):
                far = d ^ 1
                pltpu.make_async_remote_copy(
                    src_ref=table.at[pl.ds(lo, n)],
                    dst_ref=table.at[pl.ds((far + 1) * BR + lo, n)],
                    send_sem=send.at[d],
                    recv_sem=recv.at[far],
                    device_id=nearby[d],
                    device_id_type=MESH,
                ).start()

    def halo_wait(table, send, recv):
        for d in range(6):
            @pl.when(exists[d])
            def _(d=d):
                copy = pltpu.make_async_remote_copy(
                    src_ref=table.at[pl.ds(0, BR)],
                    dst_ref=table.at[pl.ds((d + 1) * BR, BR)],
                    send_sem=send.at[d],
                    recv_sem=recv.at[d],
                    device_id=nearby[d],
                    device_id_type=MESH,
                )
                copy.wait_recv()
                copy.wait_send()

    def line_copies(ref, peer, size, send, recv):
        return [
            pltpu.make_async_remote_copy(
                src_ref=ref, dst_ref=ref, send_sem=send.at[d - 1], recv_sem=recv.at[d - 1],
                device_id=peer(d), device_id_type=MESH,
            )
            for d in range(1, size)
        ]

    def go(copies):
        for copy in copies:
            copy.start()

    def done(copies):
        for copy in copies:
            copy.wait()

    halo_send(x0, xs_sem.at[0], xr_sem.at[0], 0, BR)
    cg1 = line_copies(cg.at[pl.ds(me, 1)], peer_z, NZ, c1s, c1r)
    cg2 = line_copies(cg.at[pl.ds((ix * NY + iy) * NZ, NZ)], peer_xy, NX * NY, c2s, c2r)
    go(cg1)


    def fill(r, carry):
        for j in range(4):
            b = 4 * r + j
            for s in range(NS):
                pt[b, s:s + 1, :] = p0[s, pl.ds(b, 1), :]
            pt[b, NS:8, :] = jnp.full((8 - NS, B), ids[b].astype(F32), F32)
        return carry

    sub = lax.broadcasted_iota(jnp.int32, (B, B), 0)
    lane = lax.broadcasted_iota(jnp.int32, (B, B), 1)

    def lane_sums(block):
        return jnp.sum(block.T, axis=0, keepdims=True)

    def multiply(cur, b, first):
        total = None
        for k in range(0 if first else 1, K):
            block = a_v[b, k]
            if first and k == 0:
                diag = jnp.sum(jnp.where(sub == lane, block, 0.0), axis=0, keepdims=True)
                invd[b] = 1.0 / diag
            term = block * cur[cols[k, b]]
            total = term if total is None else total + term
        return total

    def finish(nxt, b, j, first, squares):
        y = lane_sums(acc[j])
        if not first:
            y = y + own[b]
        y = y * invd[b]
        nxt[b] = y
        return squares + y * y

    def iterate(par, first, last):
        cur, nxt = (x0, x1) if par == 0 else (x1, x0)
        halo_wait(cur, xs_sem.at[par], xr_sem.at[par])
        send = functools.partial(halo_send, nxt, xs_sem.at[1 - par], xr_sem.at[1 - par])
        if not first:
            squares = jnp.zeros((1, B), F32)
            for lo, hi in ((0, 44), (44, BR)):
                for b in range(lo, hi):
                    y = (lane_sums(multiply(cur, b, first)) + own[b]) * invd[b]
                    nxt[b] = y
                    squares = squares + y * y
                if not last:
                    send(lo, hi - lo)
            return squares
        if first:
            a_copy(0).wait()
            a_copy(1).wait()
        for j in range(G):
            acc[j] = multiply(cur, j, first)

        def stage(g, squares):
            if first:
                a_copy(2 * g).wait()
                a_copy(2 * g + 1).wait()
            for j in range(G):
                squares = finish(nxt, (g - 1) * G + j, j, first, squares)
                acc[j] = multiply(cur, g * G + j, first)
            return squares

        squares = jnp.zeros((1, B), F32)
        squares = lax.fori_loop(1, 4, stage, squares)
        if not last:
            send(0, 3 * G)
        squares = lax.fori_loop(4, FULL, stage, squares)
        if first:
            a_copy(2 * FULL).wait()
        for j in range(G):
            squares = finish(nxt, (FULL - 1) * G + j, j, first, squares)
            if j < BR - FULL * G:
                acc[j] = multiply(cur, FULL * G + j, first)
        if not last:
            send(3 * G, 3 * G)
        for j in range(BR - FULL * G):
            squares = finish(nxt, FULL * G + j, j, first, squares)
        if not last:
            send(FULL * G, BR - FULL * G)
        return squares

    nt = (((1,), (1,)), ((), ()))

    def halves(value):
        high = value.astype(jnp.bfloat16)
        return high, (value - high.astype(F32)).astype(jnp.bfloat16)

    def p_row(b):
        scale = -invd[b]
        for k in range(K):
            p_hi, p_lo = halves(pt[cols[k, b]])
            p_all = jnp.concatenate([p_hi, p_lo], axis=0)
            a_all = jnp.concatenate(halves(a_v[b, k]), axis=1)
            value = lax.dot_general(
                jnp.concatenate([p_all, p_all], axis=1), a_all, nt, preferred_element_type=F32
            )
            value = (value[0:8] + value[8:16]) * scale
            for s in range(NS):
                prod[k, s, pl.ds(b, 1), :] = value[s:s + 1]

    def own_rows(cur, lo, n):
        for j in range(n):
            own[lo + j] = lane_sums(a_v[lo + j, 0] * cur[lo + j])

    def own_only(cur):
        def one(r, carry):
            own_rows(cur, r * 13, 13)
            return carry

        lax.fori_loop(0, BR // 13, one, 0)

    def between(cur, turn):
        def one(r, carry):
            p_row(turn * PROWS + r)
            own_rows(cur, jnp.minimum(r * OWN, BR - OWN), OWN)
            return carry

        lax.fori_loop(0, PROWS, one, 0)

    iterate(0, True, False)
    done(cg1)
    go(cg2)

    def two(i, carry):
        @pl.when(i == 0)
        def _():
            lax.fori_loop(0, BR // 4, fill, 0)
            halo_send(pt, ps_sem, pr_sem, 0, BR // 2)
            own_only(x1)

        @pl.when(i > 0)
        def _():
            between(x1, 2 * i - 2)

        iterate(1, False, False)

        @pl.when(i == 0)
        def _():
            halo_send(pt, ps_sem, pr_sem, BR // 2, BR // 2)
            own_only(x0)

        @pl.when(i > 0)
        def _():
            between(x0, 2 * i - 1)

        sq[0] = iterate(0, False, False)

        @pl.when(i == 0)
        def _():
            halo_wait(pt, ps_sem, pr_sem)

        return carry

    lax.fori_loop(0, (ITERS - 2) // 2, two, 0)
    done(cg2)
    between(x1, ITERS - 4)
    sq[1] = iterate(1, False, True)

    both = jnp.sum(sq[...], axis=2, keepdims=True)
    spot = lax.broadcasted_iota(jnp.int32, (1, B), 1)
    r1[iz] = jnp.where(spot < B // 2, both[0], both[1])
    red1 = line_copies(r1.at[iz], peer_z, NZ, n1s, n1r)
    go(red1)

    for b in range(PROWS * (ITERS - 3), BR):
        p_row(b)
    out = [pltpu.make_async_copy(prod, prod_out, out_sem.at[0])]
    out[0].start()

    done(red1)
    r2[ix * NY + iy] = jnp.sum(r1[...], axis=0)
    red2 = line_copies(r2.at[ix * NY + iy], peer_xy, NX * NY, n2s, n2r)
    go(red2)

    strides = (0, -NY * NZ, NY * NZ, -NZ, NZ, -1, 1)
    table = cg[:, 0, :]
    device = lax.broadcasted_iota(jnp.int32, (NX * NY * NZ, B), 0)
    for f in range(7):
        below = jnp.where(device < me + strides[f], table, 0.0)
        offs[f] = jnp.sum(below, axis=0, keepdims=True)

    def col_rows(r, carry):
        for j in range(4):
            b = 4 * r + j
            total = jnp.zeros((1, B), F32)
            for k in range(K):
                c = cols[k, b]
                face = lax.shift_right_logical(c * 1261, 16)
                value = pt[c, NS:NS + 1, :] + offs[face]
                total = jnp.where(spot == k, value, total)
            coltab[pl.ds(b, 1), :] = 6.0 * total
            zlast[pl.ds(b, 1), :] = x0[b]
        return carry

    lax.fori_loop(0, BR // 4, col_rows, 0)
    pcols[...] = coltab[...].T[0:K, 0:BR].astype(jnp.int32)
    out.append(pltpu.make_async_copy(pcols, pcols_out, out_sem.at[1]))
    out.append(pltpu.make_async_copy(zlast, z_out, out_sem.at[2]))
    out[1].start()
    out[2].start()

    done(red2)
    total = jnp.sum(r2[...], axis=0)
    norms[...] = total
    out.append(pltpu.make_async_copy(norms, norms_out, out_sem.at[3]))
    out[3].start()
    for copy in out:
        copy.wait()


def scaled(
    prod, pcols, z, norms, p0, p_blocks, p_cols, power_vec,
    prod_v, pcols_v, z_v, norms_v, p0_v, in_sem, out_sem,
):
    def taken(i, far, near):
        return pltpu.make_async_copy(far, near, in_sem.at[i])

    def given(i, near, far):
        return pltpu.make_async_copy(near, far, out_sem.at[i])

    whole = [
        taken(K + i, far, near)
        for i, (far, near) in enumerate(((norms, norms_v), (p0, p0_v), (z, z_v), (pcols, pcols_v)))
    ]
    parts = [taken(k, prod.at[k], prod_v.at[k]) for k in range(K)]
    for copy in whole[:2] + parts + whole[2:]:
        copy.start()
    whole[0].wait()
    last_norm = jnp.sqrt(norms_v[:, B - 1:B])
    spectral = last_norm / jnp.sqrt(norms_v[:, 0:1])
    entries = NX * NY * NZ * BR * B
    rescale = jnp.sqrt(F32(entries)) / last_norm
    damping = 4.0 / (3.0 * spectral)
    whole[1].wait()
    results = []
    for k in range(K):
        parts[k].wait()
        for s in range(NS):
            value = damping * prod_v[k, s]
            prod_v[k, s] = value + p0_v[s] if k == 0 else value
        results.append(given(k, prod_v.at[k], p_blocks.at[k]))
        results[k].start()
    whole[2].wait()
    z_v[...] = z_v[...] * rescale
    results.append(given(K, z_v, power_vec))
    results[K].start()
    whole[3].wait()
    results.append(given(K + 1, pcols_v, p_cols))
    results[K + 1].start()
    for copy in results:
        copy.wait()


def local(a_blocks, block_cols, agg_ids, agg_counts, p0_blocks, start_vec):
    hbm = pl.BlockSpec(memory_space=pltpu.HBM)
    anywhere = pl.BlockSpec(memory_space=pl.ANY)
    dma = pltpu.SemaphoreType.DMA
    p0_turned = jnp.transpose(p0_blocks, (1, 0, 2))
    shapes = (
        jax.ShapeDtypeStruct((K, NS, BR, B), F32),
        jax.ShapeDtypeStruct((K, BR), jnp.int32),
        jax.ShapeDtypeStruct((BR, B), F32),
    )
    prod, pcols, zlast, norms = pl.pallas_call(
        kernel,
        out_shape=(*shapes, jax.ShapeDtypeStruct((1, B), F32)),
        in_specs=[hbm, hbm, pl.BlockSpec(memory_space=pltpu.SMEM), hbm, hbm, hbm],
        out_specs=(anywhere,) * 4,
        scratch_shapes=[
            pltpu.SMEM((K, BR), jnp.int32),
            pltpu.SMEM((BR,), jnp.int32),
            pltpu.VMEM((NS, BR, B), F32),
            pltpu.VMEM((BR, B), F32),
            pltpu.VMEM((BR, K, B, B), F32),
            pltpu.VMEM((7 * BR, 1, B), F32),
            pltpu.VMEM((7 * BR, 1, B), F32),
            pltpu.VMEM((G, B, B), F32),
            pltpu.VMEM((7 * BR, 8, B), F32),
            pltpu.VMEM((K, NS, BR, B), F32),
            pltpu.VMEM((BR, 1, B), F32),
            pltpu.VMEM((BR, 1, B), F32),
            pltpu.VMEM((2, 1, B), F32),
            pltpu.VMEM((7, 1, B), F32),
            pltpu.VMEM((NX * NY * NZ, 1, B), F32),
            pltpu.VMEM((NZ, 1, B), F32),
            pltpu.VMEM((NX * NY, 1, B), F32),
            pltpu.VMEM((B, B), F32),
            pltpu.VMEM((K, BR), jnp.int32),
            pltpu.VMEM((BR, B), F32),
            pltpu.VMEM((1, B), F32),
            dma((4,)),
            dma((BR // HALF,)),
            dma((2, 6)),
            dma((2, 6)),
            dma((6,)),
            dma((6,)),
            dma((4,)),
            dma((NZ - 1,)), dma((NZ - 1,)),
            dma((NX * NY - 1,)), dma((NX * NY - 1,)),
            dma((NZ - 1,)), dma((NZ - 1,)),
            dma((NX * NY - 1,)), dma((NX * NY - 1,)),
        ],
        compiler_params=pltpu.CompilerParams(
            collective_id=0, has_side_effects=True, vmem_limit_bytes=67_043_328
        ),
        name="prolongator",
    )(block_cols.T, agg_ids, agg_counts, a_blocks, p0_turned, start_vec)
    p_blocks, p_cols, power_vec = pl.pallas_call(
        scaled,
        out_shape=shapes,
        in_specs=[hbm] * 5,
        out_specs=(hbm,) * 3,
        scratch_shapes=[
            pltpu.VMEM((K, NS, BR, B), F32),
            pltpu.VMEM((K, BR), jnp.int32),
            pltpu.VMEM((BR, B), F32),
            pltpu.VMEM((1, B), F32),
            pltpu.VMEM((NS, BR, B), F32),
            dma((K + 4,)),
            dma((K + 2,)),
        ],
        compiler_params=pltpu.CompilerParams(vmem_limit_bytes=67_043_328),
        name="scaled",
    )(prod, pcols, zlast, norms, p0_turned)
    return jnp.transpose(p_blocks, (2, 0, 1, 3)), p_cols.T, power_vec


def solution(mesh):
    placed = (
        P(AXES, None, None, None),
        P(AXES, None),
        P(AXES),
        P(AXES),
        P(AXES, None, None),
        P(AXES, None),
    )
    return jax.shard_map(
        local,
        mesh=mesh,
        in_specs=placed,
        out_specs=(P(AXES, None, None, None), P(AXES, None), P(AXES, None)),
        check_vma=False,
    )
```
